256 devices in a mesh: dp: 8 (over z_hi, x), tensor: 8 (over z_lo, core), fsdp: 4 (over y).
Axes of the slice: x: 4, y: 4, z: 8 (z_hi: 2, z_lo: 4; z = z_hi * 4 + z_lo), core: 2. Of those that a mesh axis runs over, the one named last changes fastest.
Arguments:
- train_acts: bfloat16 [8192, 4096], P(('dp', 'fsdp'), 'tensor'), may hold values from -6 to 6
- val_acts: bfloat16 [8192, 4096], P(('dp', 'fsdp'), 'tensor'), may hold values from -6 to 6
- train_cot: bfloat16 [8192, 4096], P(('dp', 'fsdp'), 'tensor'), may hold values from -6 to 6
- val_cot: bfloat16 [8192, 4096], P(('dp', 'fsdp'), 'tensor'), may hold values from -6 to 6
- train_lengths: int32 [128], P(('dp', 'fsdp')), may hold values from 16 to 64
- val_lengths: int32 [128], P(('dp', 'fsdp')), may hold values from 16 to 64
- gate_weight: bfloat16 [4096, 11008], P(('dp', 'fsdp'), 'tensor'), may hold values from -0.09375 to 0.09375
- up_weight: bfloat16 [4096, 11008], P(('dp', 'fsdp'), 'tensor'), may hold values from -0.09375 to 0.09375
- in_basis: bfloat16 [11008, 64], P('tensor'), may hold values from -0.0546875 to 0.0546875
- out_basis: bfloat16 [4096, 128], P('tensor'), may hold values from -0.09375 to 0.09375
Outputs:
- scores: float32 [128, 128], P(('dp', 'fsdp'))
The draws below stay inside these ranges and needn't reach their ends.
Inputs may be any that keep to these rules, and one draw needn't show every extreme that they name: `train_lengths`: an example's first length slots hold its tokens, the rest are padding. `val_lengths`: as for the training examples.
All inputs are finite; a program needn't handle non-finite values.
Results may differ from the reference program's by a relative error of at most 0.004.
Values may be sent and summed in bfloat16 or wider, within the bound.
A program may use at most 128 MiB of HBM per device.

```python
import jax
import jax.numpy as jnp
from jax import lax

D = 4096
FF = 11008
K_IN = 64
K_OUT = 128
SEQ = 64
TRAIN = 128
VAL = 128


def touch_ends(entries, key, low, largest):
    longest = entries.shape.index(max(entries.shape))
    spots = []
    for shift in (0, 1):
        where = [jax.random.randint(jax.random.fold_in(key, axis), (), 0, length) for axis, length in enumerate(entries.shape)]
        where[longest] = (where[longest] + shift) % entries.shape[longest]
        spots.append(tuple(where))
    return entries.at[spots[0]].set(low).at[spots[1]].set(largest)


def shard_levels(key, dims, split, low, largest):
    loudness, own = 1.0, jax.random.fold_in(key, 6)
    for dim, shards_of in split:
        heights = jnp.exp(jax.random.uniform(jax.random.fold_in(own, dim), (shards_of,), jnp.float32, low / len(split), largest / len(split)))
        loudness = loudness * jnp.repeat(heights, dims[dim] // shards_of).reshape([-1 if axis == dim else 1 for axis in range(len(dims))])
    return loudness


def scatter_about(rng, dims, width, limit, cuts=(), kind=jnp.bfloat16):
    level = shard_levels(rng, dims, cuts, -0.22, 0.18) if cuts else 1.0
    values = jax.random.normal(rng, dims, jnp.float32) * width * level
    return jnp.minimum(jnp.maximum(values, -limit), limit).astype(kind)


def setup_inputs(seed: int = 0) -> dict:
    splits = jax.random.split(jax.random.key(seed), 11)
    train_acts = scatter_about(splits[0], (TRAIN * SEQ, D), 1.0, 6.0, ((0, 32), (1, 8)))
    val_acts = scatter_about(splits[1], (VAL * SEQ, D), 1.0, 6.0, ((0, 32), (1, 8)))
    train_cot = scatter_about(splits[2], (TRAIN * SEQ, D), 1.0, 6.0, ((0, 32), (1, 8)))
    val_cot = scatter_about(splits[3], (VAL * SEQ, D), 1.0, 6.0, ((0, 32), (1, 8)))
    train_lengths = touch_ends(jax.random.randint(splits[4], (TRAIN,), SEQ // 4, SEQ + 1), jax.random.fold_in(splits[4], 1), SEQ // 4, SEQ).astype(jnp.int32)
    val_lengths = touch_ends(jax.random.randint(splits[5], (VAL,), SEQ // 4, SEQ + 1), jax.random.fold_in(splits[5], 1), SEQ // 4, SEQ).astype(jnp.int32)
    gate_weight = scatter_about(splits[6], (D, FF), D ** -0.5, 0.09375, ((0, 32), (1, 8)))
    up_weight = scatter_about(splits[7], (D, FF), D ** -0.5, 0.09375, ((0, 32), (1, 8)))
    in_basis = scatter_about(splits[8], (FF, K_IN), FF ** -0.5, 0.0546875, ((0, 8),))
    out_basis = scatter_about(splits[9], (D, K_OUT), D ** -0.5, 0.09375, ((0, 8),))
    return dict(train_acts=train_acts, val_acts=val_acts, train_cot=train_cot, val_cot=val_cot, train_lengths=train_lengths, val_lengths=val_lengths, gate_weight=gate_weight, up_weight=up_weight, in_basis=in_basis, out_basis=out_basis)


def sketch_rows(activations, cotangents, lengths, gate_weight, up_weight, in_basis, out_basis):
    gate_sum = jnp.dot(activations, gate_weight, preferred_element_type=jnp.float32)
    up_sum = jnp.dot(activations, up_weight, preferred_element_type=jnp.float32)
    hidden = (jax.nn.silu(gate_sum) * up_sum).astype(jnp.bfloat16)
    in_proj = jnp.dot(hidden, in_basis, preferred_element_type=jnp.float32)
    out_proj = jnp.dot(cotangents, out_basis, preferred_element_type=jnp.float32)
    valid = (jnp.arange(SEQ, dtype=jnp.int32)[None, :] < lengths[:, None]).astype(jnp.float32)
    in_three = in_proj.reshape(-1, SEQ, K_IN) * valid[:, :, None]
    out_three = out_proj.reshape(-1, SEQ, K_OUT)
    sketch = jnp.einsum('esj,esk->ejk', in_three, out_three, precision=lax.Precision.HIGHEST)
    sketch = sketch.reshape(sketch.shape[0], K_IN * K_OUT)
    return sketch * lax.rsqrt(lax.optimization_barrier(jnp.sum(sketch * sketch, axis=1, keepdims=True)) + 1e-06)

def reference(train_acts, val_acts, train_cot, val_cot, train_lengths, val_lengths, gate_weight, up_weight, in_basis, out_basis):
    train_unit = sketch_rows(train_acts, train_cot, train_lengths, gate_weight, up_weight, in_basis, out_basis)
    val_unit = sketch_rows(val_acts, val_cot, val_lengths, gate_weight, up_weight, in_basis, out_basis)
    product = jnp.dot(train_unit, val_unit.T, precision=lax.Precision.HIGHEST, preferred_element_type=jnp.float32)
    return product * jnp.sqrt(jnp.float32(K_IN * K_OUT))
```

```python
import jax
import jax.numpy as jnp
from jax import lax
from jax.experimental import pallas as pl
from jax.experimental.pallas import tpu as pltpu
from jax.sharding import PartitionSpec as P

SEQ = 64
MESH = pl.DeviceIdType.MESH
F32 = jnp.float32
BF16 = jnp.bfloat16
WIDE = 640
REST = 48
COLS = 1408
PLUS, MINUS = 1, -1


def mod(value, n):
    return lax.rem(value + n, n)


def body(
    tlen, vlen, gate, up, tacts, vacts, tcot, vcot, ibasis, obasis,
    out,
    wf, fx, relay, xf, acc, b2, proj, opart, orecv, osum, otr, ova,
    toward, kept, given, irecv, tbuf, vbuf, row, obuf,
    wsend, wrecv, zsend, zrecv, dsend, drecv, tsend, trecv,
):
    dp = lax.axis_index("dp")
    t = lax.axis_index("tensor")
    y = lax.axis_index("fsdp")
    zh = dp // 4
    x = lax.rem(dp, 4)
    zl = t // 2
    c = lax.rem(t, 2)
    z = zh * 4 + zl
    peer = 1 - c

    def at_z(zz, cc):
        return {"dp": (zz // 4) * 4 + x, "tensor": lax.rem(zz, 4) * 2 + cc, "fsdp": y}

    def at_xy(xx, yy):
        return {"dp": zh * 4 + xx, "tensor": t, "fsdp": yy}

    def copy(src, dst, sends, recvs, n, device):
        return pltpu.make_async_remote_copy(
            src_ref=src, dst_ref=dst, send_sem=sends.at[n], recv_sem=recvs.at[n],
            device_id=device, device_id_type=MESH,
        )

    started = []

    def start(c_):
        c_.start()
        started.append(c_)

    barrier = pltpu.get_barrier_semaphore()
    for dx in range(4):
        for dy in range(4):
            if dx or dy:
                pl.semaphore_signal(
                    barrier, inc=1, device_id=at_xy(lax.rem(x + dx, 4), lax.rem(y + dy, 4)),
                    device_id_type=MESH)
    for k in range(8):
        for cc in (c, peer):
            if k or cc is peer:
                pl.semaphore_signal(
                    barrier, inc=1, device_id=at_z(lax.rem(z + k, 8), cc), device_id_type=MESH)

    pick_r = lax.broadcasted_iota(jnp.int32, (96, 128), 0)
    pick_l = lax.broadcasted_iota(jnp.int32, (96, 128), 1)

    def pack(half):
        first = pl.multiple_of(half * WIDE, 128)
        pick_gate = (pick_l < REST) & (pick_r == pick_l + REST * half)
        pick_up = (pick_l >= 64) & (pick_l < 64 + REST) & (pick_r == pick_l - 64 + REST * half)
        rest = jnp.dot(gate[:, 1280:1376], pick_gate.astype(F32).astype(BF16), preferred_element_type=F32)
        rest += jnp.dot(up[:, 1280:1376], pick_up.astype(F32).astype(BF16), preferred_element_type=F32)
        return gate[:, pl.ds(first, WIDE)], up[:, pl.ds(first, WIDE)], rest.astype(BF16)

    fx[:, 0:WIDE], fx[:, WIDE : 2 * WIDE], fx[:, 2 * WIDE : COLS] = pack(1 - zh)
    mine = pl.ds(pl.multiple_of(y * 128, 128), 128)
    wf[dp, mine, 0:WIDE], wf[dp, mine, WIDE : 2 * WIDE], wf[dp, mine, 2 * WIDE : COLS] = pack(zh)
    pl.semaphore_wait(barrier, 30)

    def w_rows(zc, xx, yy, first, count):
        return wf.at[zc * 4 + xx, pl.ds(pl.multiple_of(yy * 128 + first, 32), count), :]

    def exchange(sign):
        n = 0 if sign == PLUS else 1
        start(copy(fx.at[pl.ds(64 * n, 64), :], relay.at[n], zsend, zrecv, n,
                   at_z(mod(z + 2 * sign, 8), c)))

    def exchange_on(sign):
        n = 0 if sign == PLUS else 1
        arrive = copy(relay.at[n], relay.at[n], zsend, zrecv, n, at_z(z, peer))
        arrive.wait_recv()
        origin = mod(z - 2 * sign, 8)
        slot = w_rows(origin // 4, x, y, 64 * n, 64)
        start(copy(relay.at[n], slot, zsend, zrecv, 2 + n, at_z(mod(z + 2 * sign, 8), c)))

    def exchanged(sign):
        n = 0 if sign == PLUS else 1
        slot = w_rows(1 - zh, x, y, 64 * n, 64)
        copy(slot, slot, zsend, zrecv, 2 + n, at_z(z, peer)).wait_recv()

    def act_slot(zz, cc, kind):
        return xf.at[lax.rem(zz, 4) * 2 + cc, zz // 4, kind]

    def kind_of(sign, n):
        return n % 2 if sign == PLUS else 1 - n % 2

    def act_send(sign, n):
        kind = kind_of(sign, n)
        base = 4 if sign == PLUS else 11
        slot = act_slot(mod(z - sign * (n // 2), 8), c, kind)
        src = slot if n > 1 else (tacts if kind == 0 else vacts)
        start(copy(src, slot, zsend, zrecv, base + n, at_z(mod(z + sign, 8), c)))

    def hand_over(slot, src, n):
        start(copy(src, slot, dsend, drecv, n, at_z(z, peer)))

    def act_arrive(sign, n):
        base = 4 if sign == PLUS else 11
        slot = act_slot(mod(z - sign * (n // 2 + 1), 8), c, kind_of(sign, n))
        copy(slot, slot, zsend, zrecv, base + n, at_z(z, peer)).wait_recv()
        if n + 2 < 7:
            act_send(sign, n + 2)
        hand_over(slot, slot, 2 + (n if sign == PLUS else 7 + n))

    def handed():
        for kind in range(2):
            slot = act_slot(z, peer, kind)
            copy(slot, slot, dsend, drecv, kind, at_z(z, peer)).wait_recv()
        for sign in (PLUS, MINUS):
            for n in range(7):
                slot = act_slot(mod(z - sign * (n // 2 + 1), 8), peer, kind_of(sign, n))
                copy(slot, slot, dsend, drecv, 2 + (n if sign == PLUS else 7 + n),
                     at_z(z, peer)).wait_recv()

    def w_part(cls, axis, da, db, part, half):
        xx, yy = (mod(x + da, 4), mod(y + db, 4)) if axis == 0 else (mod(x + db, 4), mod(y + da, 4))
        zc = zh if cls == 0 else 1 - zh
        if half is None:
            return w_rows(zc, xx, yy, 64 * part, 64)
        return w_rows(zc, xx, yy, 64 * part + 32 * half, 32)

    def w_where(cls, axis, sign, name, shift):
        first, second = axis, 1 - axis
        half = 0 if sign == PLUS else 1
        da, db, part, cut = {
            0: (0, 0, first, None), 1: (0, 0, second, None), 2: (-sign, 0, first, half),
            3: (0, -1, second, None), 4: (0, 1, second, None), 5: (0, 2, second, None),
            6: (-sign, 0, second, half), 7: (-sign, -1, second, half),
            8: (-sign, 1, second, half), 9: (-sign, 2, second, half),
        }[name]
        return w_part(cls, axis, da - shift * sign, db, part, cut)

    def w_id(cls, axis, sign, name):
        return ((cls * 2 + axis) * 2 + (0 if sign == PLUS else 1)) * 10 + name

    def w_send(cls, axis, sign, name):
        ref = w_where(cls, axis, sign, name, 0)
        to = at_xy(mod(x + sign, 4), y) if axis == 0 else at_xy(x, mod(y + sign, 4))
        start(copy(ref, ref, wsend, wrecv, w_id(cls, axis, sign, name), to))

    def w_arrive(cls, axis, sign, name):
        ref = w_where(cls, axis, sign, name, 1)
        copy(ref, ref, wsend, wrecv, w_id(cls, axis, sign, name), at_z(z, peer)).wait_recv()

    ways = [(axis, sign) for axis in (0, 1) for sign in (PLUS, MINUS)]

    def round_0(cls):
        for name in (0, 1):
            for axis, sign in ways:
                w_send(cls, axis, sign, name)

    def round_1(cls):
        for axis, sign in ways:
            w_arrive(cls, axis, sign, 0)
            w_send(cls, axis, sign, 2)
            for other in (PLUS, MINUS):
                w_send(cls, 1 - axis, other, 3 if sign == PLUS else 4)

    def round_2(cls):
        for axis, sign in ways:
            w_arrive(cls, axis, sign, 1)
            w_send(cls, axis, sign, 6)

    def round_3(cls):
        for axis in (0, 1):
            w_arrive(cls, axis, PLUS, 2)
            w_arrive(cls, axis, MINUS, 2)
            for other in (PLUS, MINUS):
                w_send(cls, 1 - axis, other, 5)

    def round_4(cls):
        for name in (3, 4):
            for axis, sign in ways:
                w_arrive(cls, axis, sign, name)
                w_send(cls, axis, sign, name + 4)

    def round_5(cls):
        for axis, sign in ways:
            w_arrive(cls, axis, sign, 5)
            w_send(cls, axis, sign, 9)

    def round_6(cls):
        for name in (6, 7, 8, 9):
            for axis, sign in ways:
                w_arrive(cls, axis, sign, name)

    exchange(PLUS)
    exchange(MINUS)
    round_0(0)
    act_send(PLUS, 0)
    act_send(MINUS, 0)
    hand_over(act_slot(z, c, 0), tacts, 0)
    hand_over(act_slot(z, c, 1), vacts, 1)
    xf[t, zh, 0] = tacts[...]
    xf[t, zh, 1] = vacts[...]

    slots = lax.broadcasted_iota(jnp.int32, (SEQ, 128), 0)
    for kind, (cot, lens) in enumerate(((tcot, tlen), (vcot, vlen))):
        value = jnp.dot(cot[...], obasis[...], preferred_element_type=F32)
        for i in range(4):
            rows = value[i * SEQ : (i + 1) * SEQ]
            opart[2 * i + kind] = jnp.where(slots < lens[i], rows, 0.0)
    dup_r = lax.broadcasted_iota(jnp.int32, (64, 128), 0)
    dup_l = lax.broadcasted_iota(jnp.int32, (64, 128), 1)
    dup = ((dup_l == dup_r) | (dup_l == dup_r + 64)).astype(F32).astype(BF16)
    main = ibasis[pl.ds(pl.multiple_of(zh * WIDE, 128), WIDE), :]
    rest = ibasis[pl.ds(pl.multiple_of(2 * WIDE + zh * REST, 16), REST), :]
    b2[0:WIDE] = jnp.dot(main, dup, preferred_element_type=F32).astype(BF16)
    b2[WIDE : WIDE + REST] = jnp.dot(rest, dup, preferred_element_type=F32).astype(BF16)
    b2[WIDE + REST : 768] = jnp.zeros((768 - WIDE - REST, 128), BF16)
    for k in range(1, 8):
        to = lax.rem(t + k, 8)
        start(copy(opart.at[to], orecv.at[t], tsend, trecv, k - 1,
                   {"dp": dp, "tensor": to, "fsdp": y}))
    orecv[t] = opart[t]

    round_1(0)
    round_2(0)
    exchange_on(PLUS)
    exchange_on(MINUS)
    act_send(PLUS, 1)
    act_send(MINUS, 1)
    round_3(0)
    for sign in (PLUS, MINUS):
        act_arrive(sign, 0)
    round_4(0)

    for k in range(1, 8):
        slot = orecv.at[mod(t - k, 8)]
        copy(slot, slot, tsend, trecv, k - 1, at_z(z, peer)).wait_recv()
    total = orecv[0]
    for k in range(1, 8):
        total += orecv[k]
    osum[...] = total
    klass = zh * 4 + zl
    train_share = copy(osum, otr, tsend, trecv, 7, at_z(z, peer))
    val_shares = []
    for zz in range(2):
        val_shares.append(copy(osum, ova, tsend, trecv, 8 + zz,
                               {"dp": zz * 4 + x, "tensor": klass, "fsdp": y}))
    own_val = [(c == 1) & (zh == zz) & (t == klass) for zz in range(2)]

    @pl.when(c == 0)
    def _():
        train_share.start()
        otr[...] = osum[...]

    for zz in range(2):
        @pl.when((c == 1) & jnp.logical_not(own_val[zz]))
        def _():
            val_shares[zz].start()

        @pl.when(own_val[zz])
        def _():
            ova[...] = osum[...]

    for sign in (PLUS, MINUS):
        act_arrive(sign, 1)
    exchanged(PLUS)
    exchanged(MINUS)
    round_0(1)
    round_5(0)
    for sign in (PLUS, MINUS):
        act_arrive(sign, 2)
    round_1(1)
    round_2(1)
    for sign in (PLUS, MINUS):
        act_arrive(sign, 3)
    round_6(0)
    round_3(1)
    for sign in (PLUS, MINUS):
        act_arrive(sign, 4)
    round_4(1)
    for sign in (PLUS, MINUS):
        act_arrive(sign, 5)
    round_5(1)
    for sign in (PLUS, MINUS):
        act_arrive(sign, 6)
    handed()
    round_6(1)

    acc[...] = jnp.zeros_like(acc)

    def step(n, carry):
        half = n // 8
        k = lax.rem(n, 8)
        a = xf[k, half].reshape(512, 512)
        acc[half] += jnp.dot(a, wf[k], preferred_element_type=F32)
        return carry

    lax.fori_loop(0, 16, step, 0)

    def silu(v):
        return v / (1.0 + jnp.exp(-v))

    def project(n, carry):
        half = n // 4
        rows = pl.ds(pl.multiple_of(lax.rem(n, 4) * 128, 128), 128)
        hidden = (silu(acc[half, rows, 0:WIDE]) * acc[half, rows, WIDE : 2 * WIDE]).astype(BF16)
        last = acc[half, rows, 2 * WIDE : COLS]
        hidden_rest = (silu(last) * pltpu.roll(last, 64, 1)).astype(BF16)
        value = jnp.dot(hidden, b2[0:WIDE], preferred_element_type=F32)
        value += jnp.dot(hidden_rest, b2[WIDE:768], preferred_element_type=F32)
        proj[half, rows, :] = value
        return carry

    lax.fori_loop(0, 8, project, 0)

    left = lax.broadcasted_iota(jnp.int32, (SEQ, 128), 1) < 64

    def message(zz, cc):
        train = proj[zz // 4, (zz % 4) * SEQ : (zz % 4 + 1) * SEQ, :]
        first = pl.multiple_of(256 + (2 * (zz % 2) + cc) * SEQ, SEQ)
        val = proj[(zz % 4) // 2, pl.ds(first, SEQ), :]
        return jnp.where(left, train, val)

    for zz in range(8):
        toward[zz] = message(zz, peer)
    start(copy(toward, given, tsend, trecv, 10, at_z(z, peer)))
    for zz in range(8):
        kept[zz] = message(zz, c)
    copy(given, given, tsend, trecv, 10, at_z(z, peer)).wait_recv()
    for zz in range(8):
        kept[zz] += given[zz]
    for k in range(1, 8):
        to = lax.rem(z + k, 8)
        start(copy(kept.at[to], irecv.at[z], tsend, trecv, 10 + k, at_z(to, c)))
    irecv[z] = kept[z]

    @pl.when(c == 1)
    def _():
        copy(otr, otr, tsend, trecv, 7, at_z(z, peer)).wait_recv()

    from_self = (zh == t // 4) & (t == lax.rem(t, 4) * 2 + 1)
    for zz in range(2):
        @pl.when((zh == zz) & jnp.logical_not(from_self))
        def _():
            copy(ova, ova, tsend, trecv, 8 + zz, at_z(z, peer)).wait_recv()

    for k in range(1, 8):
        slot = irecv.at[mod(z - k, 8)]
        copy(slot, slot, tsend, trecv, 10 + k, at_z(z, peer)).wait_recv()
    both = irecv[0]
    for k in range(1, 8):
        both += irecv[k]

    def unit(o_ref, first):
        sketch = lax.dot_general(
            both, o_ref[...], (((0,), (0,)), ((), ())),
            precision=lax.Precision.HIGHEST, preferred_element_type=F32)[first : first + 64]
        return sketch * lax.rsqrt(jnp.sum(sketch * sketch, keepdims=True) + 1e-06)

    vbuf[x * 4 + y] = unit(ova, 64).astype(BF16)
    n = 18
    for dx in range(4):
        for dy in range(4):
            if dx or dy:
                start(copy(vbuf.at[x * 4 + y], vbuf.at[x * 4 + y], tsend, trecv, n,
                           at_xy(lax.rem(x + dx, 4), lax.rem(y + dy, 4))))
                n += 1
    tbuf[zl] = unit(otr, 0)
    for k in range(1, 4):
        start(copy(tbuf.at[zl], tbuf.at[zl], tsend, trecv, 32 + k,
                   at_z(zh * 4 + lax.rem(zl + k, 4), c)))
    for k in range(1, 4):
        slot = tbuf.at[mod(zl - k, 4)]
        copy(slot, slot, tsend, trecv, 32 + k, at_z(z, peer)).wait_recv()
    n = 18
    for dx in range(4):
        for dy in range(4):
            if dx or dy:
                slot = vbuf.at[mod(x - dx, 4) * 4 + mod(y - dy, 4)]
                copy(slot, slot, tsend, trecv, n, at_z(z, peer)).wait_recv()
                n += 1

    sums = []
    for v in range(16):
        val = vbuf[v].astype(F32)
        for i in range(4):
            sums.append(jnp.sum(tbuf[i] * val, axis=0, keepdims=True))
    sums.append(jnp.zeros((64, 128), F32))
    pairs = jnp.concatenate(sums, axis=0)
    line = jnp.sum(pairs.T, axis=0, keepdims=True)
    row[...] = jnp.broadcast_to(line, (8, 128))
    for k in range(1, 8):
        to = lax.rem(t + k, 8)
        start(copy(row, obuf.at[t], tsend, trecv, 35 + k, {"dp": dp, "tensor": to, "fsdp": y}))
    obuf[t] = row[...]
    for k in range(1, 8):
        slot = obuf.at[mod(t - k, 8)]
        copy(slot, slot, tsend, trecv, 35 + k, at_z(z, peer)).wait_recv()
    out[...] = obuf[...]

    for c_ in started:
        c_.wait_send()

    @pl.when(c == 0)
    def _():
        train_share.wait_send()

    for zz in range(2):
        @pl.when((c == 1) & jnp.logical_not(own_val[zz]))
        def _():
            val_shares[zz].wait_send()


def on_device(
    train_acts, val_acts, train_cot, val_cot, train_lengths, val_lengths,
    gate_weight, up_weight, in_basis, out_basis,
):
    vmem = pl.BlockSpec(memory_space=pltpu.VMEM)
    smem = pl.BlockSpec(memory_space=pltpu.SMEM)
    dma = pltpu.SemaphoreType.DMA
    blocks = pl.pallas_call(
        body,
        out_shape=jax.ShapeDtypeStruct((8, 8, 128), F32),
        in_specs=[smem, smem] + [vmem] * 8,
        out_specs=vmem,
        scratch_shapes=[
            pltpu.VMEM((8, 512, COLS), BF16),
            pltpu.VMEM((128, COLS), BF16),
            pltpu.VMEM((2, 64, COLS), BF16),
            pltpu.VMEM((8, 2, 2, 256, 512), BF16),
            pltpu.VMEM((2, 512, COLS), F32),
            pltpu.VMEM((768, 128), BF16),
            pltpu.VMEM((2, 512, 128), F32),
            pltpu.VMEM((8, SEQ, 128), F32),
            pltpu.VMEM((8, SEQ, 128), F32),
            pltpu.VMEM((SEQ, 128), F32),
            pltpu.VMEM((SEQ, 128), F32),
            pltpu.VMEM((SEQ, 128), F32),
            pltpu.VMEM((8, SEQ, 128), F32),
            pltpu.VMEM((8, SEQ, 128), F32),
            pltpu.VMEM((8, SEQ, 128), F32),
            pltpu.VMEM((8, SEQ, 128), F32),
            pltpu.VMEM((4, 64, 128), F32),
            pltpu.VMEM((16, 64, 128), BF16),
            pltpu.VMEM((8, 128), F32),
            pltpu.VMEM((8, 8, 128), F32),
            dma((80,)), dma((80,)),
            dma((18,)), dma((18,)),
            dma((16,)), dma((16,)),
            dma((43,)), dma((43,)),
        ],
        compiler_params=pltpu.CompilerParams(
            collective_id=0, has_side_effects=True, vmem_limit_bytes=60 * 1024 * 1024
        ),
    )(train_lengths, val_lengths, gate_weight, up_weight, train_acts, val_acts,
      train_cot, val_cot, in_basis, out_basis)
    scores = blocks[:, 0, :64].reshape(2, 4, 16, 4)
    scores = scores.transpose(3, 0, 2, 1).reshape(4, 128)
    return scores * jnp.sqrt(jnp.float32(64 * 128))


def solution(mesh):
    rows = P(("dp", "fsdp"), "tensor")
    placed = (rows, rows, rows, rows, P(("dp", "fsdp")), P(("dp", "fsdp")), rows, rows,
              P("tensor", None), P("tensor", None))
    return jax.shard_map(
        on_device, mesh=mesh, in_specs=placed, out_specs=P(("dp", "fsdp"), None), check_vma=False
    )
```

```python
import jax
import jax.numpy as jnp
from jax import lax
from jax.experimental import pallas as pl
from jax.experimental.pallas import tpu as pltpu
from jax.sharding import PartitionSpec as P

SEQ = 64
MESH = pl.DeviceIdType.MESH
F32 = jnp.float32
BF16 = jnp.bfloat16
HALF = 688
SPAN = 736
CUT = 352
PLUS, MINUS = 1, -1


def mod(value, n):
    return lax.rem(value + n, n)


def body(
    tlen, vlen, gate, up, tacts, vacts, tcot, vcot, ibasis, obasis,
    out,
    wf, relay, xf, acc, hbuf, proj, opart, orecv, osum, otr, ova,
    toward, kept, given, irecv, tbuf, vbuf, row, obuf,
    wsend, wrecv, zsend, zrecv, dsend, drecv, tsend, trecv,
):
    dp = lax.axis_index("dp")
    t = lax.axis_index("tensor")
    y = lax.axis_index("fsdp")
    zh = dp // 4
    x = lax.rem(dp, 4)
    zl = t // 2
    c = lax.rem(t, 2)
    z = zh * 4 + zl
    peer = 1 - c

    def at_z(zz, cc):
        return {"dp": (zz // 4) * 4 + x, "tensor": lax.rem(zz, 4) * 2 + cc, "fsdp": y}

    def at_xy(xx, yy):
        return {"dp": zh * 4 + xx, "tensor": t, "fsdp": yy}

    def copy(src, dst, sends, recvs, n, device):
        return pltpu.make_async_remote_copy(
            src_ref=src, dst_ref=dst, send_sem=sends.at[n], recv_sem=recvs.at[n],
            device_id=device, device_id_type=MESH,
        )

    started = []

    def start(c_):
        c_.start()
        started.append(c_)

    barrier = pltpu.get_barrier_semaphore()
    near = [at_xy(mod(x + s, 4), y) for s in (1, -1)] + [at_xy(x, mod(y + s, 4)) for s in (1, -1)]
    near += [at_z(mod(z + s, 8), c) for s in (1, -1, 2, -2)] + [at_z(z, peer)]
    for device in near:
        pl.semaphore_signal(barrier, inc=1, device_id=device, device_id_type=MESH)

    weights = (gate, up)

    def own_rows(half):
        return pl.ds(pl.multiple_of(half * HALF, 16), HALF)

    for part in range(2):
        wf[dp, y, part * HALF : (part + 1) * HALF, :] = weights[part][own_rows(zh), :]
    xf[t, zh, 0] = tacts[...]
    xf[t, zh, 1] = vacts[...]
    pl.semaphore_wait(barrier, len(near))

    def w_rows(zc, xx, yy, part, half=None):
        first, count = {None: (0, HALF), 0: (0, CUT), 1: (CUT, HALF - CUT)}[half]
        return wf.at[zc * 4 + xx, yy, pl.ds(part * HALF + first, count), :]

    def exchange(sign):
        n = 0 if sign == PLUS else 1
        start(copy(weights[n].at[own_rows(1 - zh), :], relay.at[n], zsend, zrecv, n,
                   at_z(mod(z + 2 * sign, 8), c)))

    def exchange_on(sign):
        n = 0 if sign == PLUS else 1
        copy(relay.at[n], relay.at[n], zsend, zrecv, n, at_z(z, peer)).wait_recv()
        origin = mod(z - 2 * sign, 8)
        slot = w_rows(origin // 4, x, y, n)
        start(copy(relay.at[n], slot, zsend, zrecv, 2 + n, at_z(mod(z + 2 * sign, 8), c)))

    def exchanged(sign):
        n = 0 if sign == PLUS else 1
        slot = w_rows(1 - zh, x, y, n)
        copy(slot, slot, zsend, zrecv, 2 + n, at_z(z, peer)).wait_recv()

    def act_slot(zz, cc, kind):
        return xf.at[lax.rem(zz, 4) * 2 + cc, zz // 4, kind]

    def kind_of(sign, n):
        return n % 2 if sign == PLUS else 1 - n % 2

    def act_send(sign, n):
        kind = kind_of(sign, n)
        base = 4 if sign == PLUS else 11
        slot = act_slot(mod(z - sign * (n // 2), 8), c, kind)
        src = slot if n > 1 else (tacts if kind == 0 else vacts)
        start(copy(src, slot, zsend, zrecv, base + n, at_z(mod(z + sign, 8), c)))

    def hand_over(slot, src, n):
        start(copy(src, slot, dsend, drecv, n, at_z(z, peer)))

    def act_arrive(sign, n):
        base = 4 if sign == PLUS else 11
        slot = act_slot(mod(z - sign * (n // 2 + 1), 8), c, kind_of(sign, n))
        copy(slot, slot, zsend, zrecv, base + n, at_z(z, peer)).wait_recv()
        if n + 2 < 7:
            act_send(sign, n + 2)
        hand_over(slot, slot, 2 + (n if sign == PLUS else 7 + n))

    def handed_own():
        for kind in range(2):
            slot = act_slot(z, peer, kind)
            copy(slot, slot, dsend, drecv, kind, at_z(z, peer)).wait_recv()

    def handed(*steps):
        for n in steps:
            for sign in (PLUS, MINUS):
                slot = act_slot(mod(z - sign * (n // 2 + 1), 8), peer, kind_of(sign, n))
                copy(slot, slot, dsend, drecv, 2 + (n if sign == PLUS else 7 + n),
                     at_z(z, peer)).wait_recv()

    def acts(n):
        for sign in (PLUS, MINUS):
            act_arrive(sign, n)

    def w_part(cls, axis, da, db, part, half):
        xx, yy = (mod(x + da, 4), mod(y + db, 4)) if axis == 0 else (mod(x + db, 4), mod(y + da, 4))
        zc = zh if cls == 0 else 1 - zh
        return w_rows(zc, xx, yy, part, half)

    def w_where(cls, axis, sign, name, shift):
        first, second = axis, 1 - axis
        half = 0 if sign == PLUS else 1
        da, db, part, cut = {
            0: (0, 0, first, None), 1: (0, 0, second, None), 2: (-sign, 0, first, half),
            3: (0, -1, second, None), 4: (0, 1, second, None), 5: (0, 2, second, None),
            6: (-sign, 0, second, half), 7: (-sign, -1, second, half),
            8: (-sign, 1, second, half), 9: (-sign, 2, second, half),
        }[name]
        return w_part(cls, axis, da - shift * sign, db, part, cut)

    def w_id(cls, axis, sign, name):
        return ((cls * 2 + axis) * 2 + (0 if sign == PLUS else 1)) * 10 + name

    def w_send(cls, axis, sign, name):
        ref = w_where(cls, axis, sign, name, 0)
        src = ref
        if cls == 0 and name < 2:
            src = weights[axis if name == 0 else 1 - axis].at[own_rows(zh), :]
        to = at_xy(mod(x + sign, 4), y) if axis == 0 else at_xy(x, mod(y + sign, 4))
        start(copy(src, ref, wsend, wrecv, w_id(cls, axis, sign, name), to))

    def w_arrive(cls, axis, sign, name):
        ref = w_where(cls, axis, sign, name, 1)
        copy(ref, ref, wsend, wrecv, w_id(cls, axis, sign, name), at_z(z, peer)).wait_recv()

    ways = [(axis, sign) for axis in (0, 1) for sign in (PLUS, MINUS)]

    def round_0(cls):
        for name in (0, 1):
            for axis, sign in ways:
                w_send(cls, axis, sign, name)

    def round_1(cls):
        for axis, sign in ways:
            w_arrive(cls, axis, sign, 0)
            w_send(cls, axis, sign, 2)
            for other in (PLUS, MINUS):
                w_send(cls, 1 - axis, other, 3 if sign == PLUS else 4)

    def round_2(cls):
        for axis, sign in ways:
            w_arrive(cls, axis, sign, 1)
            w_send(cls, axis, sign, 6)

    def round_3(cls):
        for axis in (0, 1):
            w_arrive(cls, axis, PLUS, 2)
            w_arrive(cls, axis, MINUS, 2)
            for other in (PLUS, MINUS):
                w_send(cls, 1 - axis, other, 5)

    def round_4(cls):
        for name in (3, 4):
            for axis, sign in ways:
                w_arrive(cls, axis, sign, name)
                w_send(cls, axis, sign, name + 4)

    def round_5(cls):
        for axis, sign in ways:
            w_arrive(cls, axis, sign, 5)
            w_send(cls, axis, sign, 9)

    def round_6(cls, names=(6, 7, 8, 9)):
        for name in names:
            for axis, sign in ways:
                w_arrive(cls, axis, sign, name)

    def multiply(half, k):
        rows = jnp.concatenate([wf[k, i] for i in range(4)], axis=1)
        acc[half] += lax.dot_general(
            rows, xf[k, half].reshape(512, 512), (((1,), (1,)), ((), ())),
            preferred_element_type=F32)

    away = []
    for m in range(4):
        there = (m // 2) * 4 + 2 * zh + m % 2
        ahead = mod(there - z, 8)
        away.append(jnp.minimum(ahead, lax.rem(8 - ahead, 8)) * 4 + m)
    nearest = []
    for p in range(4):
        pick = 0
        for m in range(4):
            rank = sum((away[o] < away[m]).astype(jnp.int32) for o in range(4) if o != m)
            pick = pick + m * (rank == p).astype(jnp.int32)
        nearest.append(pick)

    def near_tasks(p):
        def step(n, carry):
            multiply(nearest[p] // 2, zh * 4 + 2 * lax.rem(nearest[p], 2) + n)
            return carry

        lax.fori_loop(0, 2, step, 0)

    def far_tasks(first, count):
        def step(n, carry):
            g = n // 2
            dx = g + (g == 2).astype(jnp.int32) - (g == 3).astype(jnp.int32)
            multiply(lax.rem(n, 2), (1 - zh) * 4 + lax.rem(x + dx, 4))
            return carry

        lax.fori_loop(first, first + count, step, 0)

    exchange(PLUS)
    exchange(MINUS)
    round_0(0)
    act_send(PLUS, 0)
    act_send(MINUS, 0)
    hand_over(act_slot(z, c, 0), tacts, 0)
    hand_over(act_slot(z, c, 1), vacts, 1)
    acc[...] = jnp.zeros_like(acc)

    slots = lax.broadcasted_iota(jnp.int32, (SEQ, 128), 0)
    for kind, (cot, lens) in enumerate(((tcot, tlen), (vcot, vlen))):
        value = jnp.dot(cot[...], obasis[...], preferred_element_type=F32)
        for i in range(4):
            rows = value[i * SEQ : (i + 1) * SEQ]
            opart[2 * i + kind] = jnp.where(slots < lens[i], rows, 0.0)
    orecv[t] = opart[t]

    round_1(0)
    round_2(0)
    exchange_on(PLUS)
    exchange_on(MINUS)
    act_send(PLUS, 1)
    act_send(MINUS, 1)
    round_3(0)
    acts(0)
    round_4(0)
    acts(1)
    exchanged(PLUS)
    exchanged(MINUS)
    round_0(1)
    round_5(0)
    acts(2)
    round_6(0)
    round_1(1)
    acts(3)
    round_2(1)
    handed_own()
    handed(0, 1, 2, 3)
    near_tasks(0)
    round_3(1)
    acts(4)
    near_tasks(1)
    round_4(1)
    acts(5)
    handed(4, 5)
    for k in range(1, 8):
        to = lax.rem(t + k, 8)
        start(copy(opart.at[to], orecv.at[t], tsend, trecv, k - 1,
                   {"dp": dp, "tensor": to, "fsdp": y}))
    near_tasks(2)
    round_5(1)
    acts(6)
    handed(6)

    for k in range(1, 8):
        slot = orecv.at[mod(t - k, 8)]
        copy(slot, slot, tsend, trecv, k - 1, at_z(z, peer)).wait_recv()
    total = orecv[0]
    for k in range(1, 8):
        total += orecv[k]
    osum[...] = total
    klass = zh * 4 + zl
    train_share = copy(osum, otr, tsend, trecv, 7, at_z(z, peer))
    val_shares = []
    for zz in range(2):
        val_shares.append(copy(osum, ova, tsend, trecv, 8 + zz,
                               {"dp": zz * 4 + x, "tensor": klass, "fsdp": y}))
    own_val = [(c == 1) & (zh == zz) & (t == klass) for zz in range(2)]

    @pl.when(c == 0)
    def _():
        train_share.start()
        otr[...] = osum[...]

    for zz in range(2):
        @pl.when((c == 1) & jnp.logical_not(own_val[zz]))
        def _():
            val_shares[zz].start()

        @pl.when(own_val[zz])
        def _():
            ova[...] = osum[...]

    near_tasks(3)
    round_6(1, (6,))
    far_tasks(0, 2)
    round_6(1, (7, 8))
    far_tasks(2, 4)
    round_6(1, (9,))
    far_tasks(6, 2)

    def silu(v):
        return v / (1.0 + jnp.exp(-v))

    basis = ibasis[:, pl.ds(pl.multiple_of(zh * 640, 128), SPAN)]
    basis = jnp.concatenate([basis, basis], axis=0)
    hbuf[0 : SPAN - HALF] = jnp.zeros((SPAN - HALF, 128), BF16)
    hbuf[HALF:SPAN] = jnp.zeros((SPAN - HALF, 128), BF16)

    def project(n, carry):
        half = n // 4
        first = pl.multiple_of(lax.rem(n, 4) * 128, 128)
        tokens = pl.ds(first, 128)
        hidden = silu(acc[half, 0:HALF, tokens]) * acc[half, HALF : 2 * HALF, tokens]
        hbuf[pl.ds(pl.multiple_of(zh * (SPAN - HALF), 16), HALF), :] = hidden.astype(BF16)
        value = jnp.dot(basis, hbuf[...], preferred_element_type=F32)
        proj[half, tokens, :] = value.T
        return carry

    lax.fori_loop(0, 8, project, 0)

    left = lax.broadcasted_iota(jnp.int32, (SEQ, 128), 1) < 64

    def message(zz, cc):
        train = proj[zz // 4, (zz % 4) * SEQ : (zz % 4 + 1) * SEQ, :]
        first = pl.multiple_of(256 + (2 * (zz % 2) + cc) * SEQ, SEQ)
        val = proj[(zz % 4) // 2, pl.ds(first, SEQ), :]
        return jnp.where(left, train, val)

    for zz in range(8):
        toward[zz] = message(zz, peer)
    start(copy(toward, given, tsend, trecv, 10, at_z(z, peer)))
    for zz in range(8):
        kept[zz] = message(zz, c)
    copy(given, given, tsend, trecv, 10, at_z(z, peer)).wait_recv()
    for zz in range(8):
        kept[zz] += given[zz]
    for k in range(1, 8):
        to = lax.rem(z + k, 8)
        start(copy(kept.at[to], irecv.at[z], tsend, trecv, 10 + k, at_z(to, c)))
    irecv[z] = kept[z]

    @pl.when(c == 1)
    def _():
        copy(otr, otr, tsend, trecv, 7, at_z(z, peer)).wait_recv()

    from_self = (zh == t // 4) & (t == lax.rem(t, 4) * 2 + 1)
    for zz in range(2):
        @pl.when((zh == zz) & jnp.logical_not(from_self))
        def _():
            copy(ova, ova, tsend, trecv, 8 + zz, at_z(z, peer)).wait_recv()

    for k in range(1, 8):
        slot = irecv.at[mod(z - k, 8)]
        copy(slot, slot, tsend, trecv, 10 + k, at_z(z, peer)).wait_recv()
    both = irecv[0]
    for k in range(1, 8):
        both += irecv[k]

    def unit(o_ref, first):
        sketch = lax.dot_general(
            both, o_ref[...], (((0,), (0,)), ((), ())),
            precision=lax.Precision.HIGHEST, preferred_element_type=F32)[first : first + 64]
        return sketch * lax.rsqrt(jnp.sum(sketch * sketch, keepdims=True) + 1e-06)

    vbuf[x * 4 + y] = unit(ova, 64).astype(BF16)
    n = 18
    for dx in range(4):
        for dy in range(4):
            if dx or dy:
                start(copy(vbuf.at[x * 4 + y], vbuf.at[x * 4 + y], tsend, trecv, n,
                           at_xy(lax.rem(x + dx, 4), lax.rem(y + dy, 4))))
                n += 1
    tbuf[zl] = unit(otr, 0)
    for k in range(1, 4):
        start(copy(tbuf.at[zl], tbuf.at[zl], tsend, trecv, 32 + k,
                   at_z(zh * 4 + lax.rem(zl + k, 4), c)))
    for k in range(1, 4):
        slot = tbuf.at[mod(zl - k, 4)]
        copy(slot, slot, tsend, trecv, 32 + k, at_z(z, peer)).wait_recv()
    n = 18
    for dx in range(4):
        for dy in range(4):
            if dx or dy:
                slot = vbuf.at[mod(x - dx, 4) * 4 + mod(y - dy, 4)]
                copy(slot, slot, tsend, trecv, n, at_z(z, peer)).wait_recv()
                n += 1

    where_r = lax.broadcasted_iota(jnp.int32, (16, 128), 0)
    where_l = lax.broadcasted_iota(jnp.int32, (16, 128), 1)
    place = where_l == where_r * 4 + (t // 4) * 64 + lax.rem(t, 4)
    vals = [vbuf[v].astype(F32) for v in range(16)]
    lines = []
    for i in range(4):
        train = tbuf[i]
        pairs = jnp.concatenate(
            [jnp.sum(train * val, axis=0, keepdims=True) for val in vals], axis=0)
        dots = jnp.sum(pairs, axis=1, keepdims=True) * jnp.sqrt(jnp.float32(64 * 128))
        lines.append(jnp.sum(jnp.where(place, dots, 0.0), axis=0, keepdims=True))
    row[...] = jnp.concatenate(lines + [jnp.zeros((4, 128), F32)], axis=0)
    for k in range(1, 8):
        to = lax.rem(t + k, 8)
        start(copy(row, obuf.at[t], tsend, trecv, 35 + k, {"dp": dp, "tensor": to, "fsdp": y}))
    obuf[t] = row[...]
    for k in range(1, 8):
        slot = obuf.at[mod(t - k, 8)]
        copy(slot, slot, tsend, trecv, 35 + k, at_z(z, peer)).wait_recv()
    scores = obuf[0]
    for k in range(1, 8):
        scores += obuf[k]
    out[...] = scores[0:4]

    for c_ in started:
        c_.wait_send()

    @pl.when(c == 0)
    def _():
        train_share.wait_send()

    for zz in range(2):
        @pl.when((c == 1) & jnp.logical_not(own_val[zz]))
        def _():
            val_shares[zz].wait_send()


def on_device(
    train_acts, val_acts, train_cot, val_cot, train_lengths, val_lengths,
    gate_weight, up_weight, in_basis, out_basis,
):
    vmem = pl.BlockSpec(memory_space=pltpu.VMEM)
    smem = pl.BlockSpec(memory_space=pltpu.SMEM)
    dma = pltpu.SemaphoreType.DMA
    return pl.pallas_call(
        body,
        out_shape=jax.ShapeDtypeStruct((4, 128), F32),
        in_specs=[smem, smem] + [vmem] * 8,
        out_specs=vmem,
        scratch_shapes=[
            pltpu.VMEM((8, 4, 2 * HALF, 128), BF16),
            pltpu.VMEM((2, HALF, 128), BF16),
            pltpu.VMEM((8, 2, 2, 256, 512), BF16),
            pltpu.VMEM((2, 2 * HALF, 512), F32),
            pltpu.VMEM((SPAN, 128), BF16),
            pltpu.VMEM((2, 512, 128), F32),
            pltpu.VMEM((8, SEQ, 128), F32),
            pltpu.VMEM((8, SEQ, 128), F32),
            pltpu.VMEM((SEQ, 128), F32),
            pltpu.VMEM((SEQ, 128), F32),
            pltpu.VMEM((SEQ, 128), F32),
            pltpu.VMEM((8, SEQ, 128), F32),
            pltpu.VMEM((8, SEQ, 128), F32),
            pltpu.VMEM((8, SEQ, 128), F32),
            pltpu.VMEM((8, SEQ, 128), F32),
            pltpu.VMEM((4, 64, 128), F32),
            pltpu.VMEM((16, 64, 128), BF16),
            pltpu.VMEM((8, 128), F32),
            pltpu.VMEM((8, 8, 128), F32),
            dma((80,)), dma((80,)),
            dma((18,)), dma((18,)),
            dma((16,)), dma((16,)),
            dma((43,)), dma((43,)),
        ],
        compiler_params=pltpu.CompilerParams(
            collective_id=0, has_side_effects=True, vmem_limit_bytes=60 * 1024 * 1024
        ),
    )(train_lengths, val_lengths, gate_weight.T, up_weight.T, train_acts, val_acts,
      train_cot, val_cot, in_basis.T, out_basis)


def solution(mesh):
    rows = P(("dp", "fsdp"), "tensor")
    placed = (rows, rows, rows, rows, P(("dp", "fsdp")), P(("dp", "fsdp")), rows, rows,
              P("tensor", None), P("tensor", None))
    return jax.shard_map(
        on_device, mesh=mesh, in_specs=placed, out_specs=P(("dp", "fsdp"), None), check_vma=False
    )
```

```python
import jax
import jax.numpy as jnp
from jax import lax
from jax.experimental import pallas as pl
from jax.experimental.pallas import tpu as pltpu
from jax.sharding import PartitionSpec as P

SEQ = 64
MESH = pl.DeviceIdType.MESH
F32 = jnp.float32
BF16 = jnp.bfloat16
HALF = 688
SPAN = 736
CUT = 352
PLUS, MINUS = 1, -1


def mod(value, n):
    return lax.rem(value + n, n)


def body(
    tlen_in, vlen_in, gate, up, tacts, vacts, tcot, vcot, ibasis_in, obasis_in,
    out,
    tlen, vlen, other, cots, ibasis, obasis, wf, relay, xf, acc, hbuf, proj, opart, orecv, osum, otr, ova,
    toward, kept, given, irecv, tbuf, vbuf, row, obuf,
    wsend, wrecv, zsend, zrecv, dsend, drecv, tsend, trecv, isem,
):
    dp = lax.axis_index("dp")
    t = lax.axis_index("tensor")
    y = lax.axis_index("fsdp")
    zh = dp // 4
    x = lax.rem(dp, 4)
    zl = t // 2
    c = lax.rem(t, 2)
    z = zh * 4 + zl
    peer = 1 - c

    def at_z(zz, cc):
        return {"dp": (zz // 4) * 4 + x, "tensor": lax.rem(zz, 4) * 2 + cc, "fsdp": y}

    def at_xy(xx, yy):
        return {"dp": zh * 4 + xx, "tensor": t, "fsdp": yy}

    def copy(src, dst, sends, recvs, n, device):
        return pltpu.make_async_remote_copy(
            src_ref=src, dst_ref=dst, send_sem=sends.at[n], recv_sem=recvs.at[n],
            device_id=device, device_id_type=MESH,
        )

    started = []

    def start(c_):
        c_.start()
        started.append(c_)

    barrier = pltpu.get_barrier_semaphore()
    near = [at_xy(mod(x + s, 4), y) for s in (1, -1)] + [at_xy(x, mod(y + s, 4)) for s in (1, -1)]
    near += [at_z(mod(z + s, 8), c) for s in (1, -1, 2, -2)] + [at_z(z, peer)]
    for device in near:
        pl.semaphore_signal(barrier, inc=1, device_id=device, device_id_type=MESH)

    def own_rows(half):
        return pl.ds(pl.multiple_of(half * HALF, 16), HALF)

    fetches = [
        (gate.at[own_rows(zh), :], wf.at[dp, y, pl.ds(0, HALF), :]),
        (up.at[own_rows(zh), :], wf.at[dp, y, pl.ds(HALF, HALF), :]),
        (gate.at[own_rows(1 - zh), :], other.at[0]), (up.at[own_rows(1 - zh), :], other.at[1]),
        (tacts, xf.at[t, zh, 0]), (vacts, xf.at[t, zh, 1]),
        (tcot, cots.at[0]), (vcot, cots.at[1]), (obasis_in, obasis), (ibasis_in, ibasis),
        (tlen_in, tlen), (vlen_in, vlen),
    ]
    fetches = [pltpu.make_async_copy(a, b, isem.at[n]) for n, (a, b) in enumerate(fetches)]
    for fetch in fetches:
        fetch.start()
    for fetch in fetches[:6]:
        fetch.wait()
    pl.semaphore_wait(barrier, len(near))

    def w_rows(zc, xx, yy, part, half=None):
        first, count = {None: (0, HALF), 0: (0, CUT), 1: (CUT, HALF - CUT)}[half]
        return wf.at[zc * 4 + xx, yy, pl.ds(part * HALF + first, count), :]

    def exchange(sign):
        n = 0 if sign == PLUS else 1
        start(copy(other.at[n], relay.at[n], zsend, zrecv, n,
                   at_z(mod(z + 2 * sign, 8), c)))

    def exchange_on(sign):
        n = 0 if sign == PLUS else 1
        copy(relay.at[n], relay.at[n], zsend, zrecv, n, at_z(z, peer)).wait_recv()
        origin = mod(z - 2 * sign, 8)
        slot = w_rows(origin // 4, x, y, n)
        start(copy(relay.at[n], slot, zsend, zrecv, 2 + n, at_z(mod(z + 2 * sign, 8), c)))

    def exchanged(sign):
        n = 0 if sign == PLUS else 1
        slot = w_rows(1 - zh, x, y, n)
        copy(slot, slot, zsend, zrecv, 2 + n, at_z(z, peer)).wait_recv()

    def act_slot(zz, cc, kind):
        return xf.at[lax.rem(zz, 4) * 2 + cc, zz // 4, kind]

    def kind_of(sign, n):
        return n % 2 if sign == PLUS else 1 - n % 2

    def act_send(sign, n):
        kind = kind_of(sign, n)
        base = 4 if sign == PLUS else 11
        slot = act_slot(mod(z - sign * (n // 2), 8), c, kind)
        start(copy(slot, slot, zsend, zrecv, base + n, at_z(mod(z + sign, 8), c)))

    def hand_over(slot, n):
        start(copy(slot, slot, dsend, drecv, n, at_z(z, peer)))

    def act_arrive(sign, n):
        base = 4 if sign == PLUS else 11
        slot = act_slot(mod(z - sign * (n // 2 + 1), 8), c, kind_of(sign, n))
        copy(slot, slot, zsend, zrecv, base + n, at_z(z, peer)).wait_recv()
        if n + 2 < 7:
            act_send(sign, n + 2)
        hand_over(slot, 2 + (n if sign == PLUS else 7 + n))

    def handed_own():
        for kind in range(2):
            slot = act_slot(z, peer, kind)
            copy(slot, slot, dsend, drecv, kind, at_z(z, peer)).wait_recv()

    def handed(*steps):
        for n in steps:
            for sign in (PLUS, MINUS):
                slot = act_slot(mod(z - sign * (n // 2 + 1), 8), peer, kind_of(sign, n))
                copy(slot, slot, dsend, drecv, 2 + (n if sign == PLUS else 7 + n),
                     at_z(z, peer)).wait_recv()

    def acts(n):
        for sign in (PLUS, MINUS):
            act_arrive(sign, n)

    def w_part(cls, axis, da, db, part, half):
        xx, yy = (mod(x + da, 4), mod(y + db, 4)) if axis == 0 else (mod(x + db, 4), mod(y + da, 4))
        zc = zh if cls == 0 else 1 - zh
        return w_rows(zc, xx, yy, part, half)

    def w_where(cls, axis, sign, name, shift):
        first, second = axis, 1 - axis
        half = 0 if sign == PLUS else 1
        da, db, part, cut = {
            0: (0, 0, first, None), 1: (0, 0, second, None), 2: (-sign, 0, first, half),
            3: (0, -1, second, None), 4: (0, 1, second, None), 5: (0, 2, second, None),
            6: (-sign, 0, second, half), 7: (-sign, -1, second, half),
            8: (-sign, 1, second, half), 9: (-sign, 2, second, half),
        }[name]
        return w_part(cls, axis, da - shift * sign, db, part, cut)

    def w_id(cls, axis, sign, name):
        return ((cls * 2 + axis) * 2 + (0 if sign == PLUS else 1)) * 10 + name

    def w_send(cls, axis, sign, name):
        ref = w_where(cls, axis, sign, name, 0)
        to = at_xy(mod(x + sign, 4), y) if axis == 0 else at_xy(x, mod(y + sign, 4))
        start(copy(ref, ref, wsend, wrecv, w_id(cls, axis, sign, name), to))

    def w_arrive(cls, axis, sign, name):
        ref = w_where(cls, axis, sign, name, 1)
        copy(ref, ref, wsend, wrecv, w_id(cls, axis, sign, name), at_z(z, peer)).wait_recv()

    ways = [(axis, sign) for axis in (0, 1) for sign in (PLUS, MINUS)]

    def round_0(cls):
        for name in (0, 1):
            for axis, sign in ways:
                w_send(cls, axis, sign, name)

    def round_1(cls):
        for axis, sign in ways:
            w_arrive(cls, axis, sign, 0)
            w_send(cls, axis, sign, 2)
            for other in (PLUS, MINUS):
                w_send(cls, 1 - axis, other, 3 if sign == PLUS else 4)

    def round_2(cls):
        for axis, sign in ways:
            w_arrive(cls, axis, sign, 1)
            w_send(cls, axis, sign, 6)

    def round_3(cls):
        for axis in (0, 1):
            w_arrive(cls, axis, PLUS, 2)
            w_arrive(cls, axis, MINUS, 2)
            for other in (PLUS, MINUS):
                w_send(cls, 1 - axis, other, 5)

    def round_4(cls):
        for name in (3, 4):
            for axis, sign in ways:
                w_arrive(cls, axis, sign, name)
                w_send(cls, axis, sign, name + 4)

    def round_5(cls):
        for axis, sign in ways:
            w_arrive(cls, axis, sign, 5)
            w_send(cls, axis, sign, 9)

    def round_6(cls, names=(6, 7, 8, 9)):
        for name in names:
            for axis, sign in ways:
                w_arrive(cls, axis, sign, name)

    def multiply(half, k):
        rows = jnp.concatenate([wf[k, i] for i in range(4)], axis=1)
        acc[half] += lax.dot_general(
            rows, xf[k, half].reshape(512, 512), (((1,), (1,)), ((), ())),
            preferred_element_type=F32)

    away = []
    for m in range(4):
        there = (m // 2) * 4 + 2 * zh + m % 2
        ahead = mod(there - z, 8)
        away.append(jnp.minimum(ahead, lax.rem(8 - ahead, 8)) * 4 + m)
    nearest = []
    for p in range(4):
        pick = 0
        for m in range(4):
            rank = sum((away[o] < away[m]).astype(jnp.int32) for o in range(4) if o != m)
            pick = pick + m * (rank == p).astype(jnp.int32)
        nearest.append(pick)

    def near_tasks(p):
        def step(n, carry):
            multiply(nearest[p] // 2, zh * 4 + 2 * lax.rem(nearest[p], 2) + n)
            return carry

        lax.fori_loop(0, 2, step, 0)

    def far_tasks(first, count):
        def step(n, carry):
            g = n // 2
            dx = g + (g == 2).astype(jnp.int32) - (g == 3).astype(jnp.int32)
            multiply(lax.rem(n, 2), (1 - zh) * 4 + lax.rem(x + dx, 4))
            return carry

        lax.fori_loop(first, first + count, step, 0)

    exchange(PLUS)
    exchange(MINUS)
    round_0(0)
    act_send(PLUS, 0)
    act_send(MINUS, 0)
    hand_over(act_slot(z, c, 0), 0)
    hand_over(act_slot(z, c, 1), 1)
    acc[...] = jnp.zeros_like(acc)

    for fetch in fetches[6:]:
        fetch.wait()
    slots = lax.broadcasted_iota(jnp.int32, (SEQ, 128), 0)
    for kind, lens in enumerate((tlen, vlen)):
        value = jnp.dot(cots[kind], obasis[...], preferred_element_type=F32)
        for i in range(4):
            rows = value[i * SEQ : (i + 1) * SEQ]
            opart[2 * i + kind] = jnp.where(slots < lens[i], rows, 0.0)
    orecv[t] = opart[t]

    round_1(0)
    round_2(0)
    exchange_on(PLUS)
    exchange_on(MINUS)
    act_send(PLUS, 1)
    act_send(MINUS, 1)
    round_3(0)
    acts(0)
    round_4(0)
    acts(1)
    exchanged(PLUS)
    exchanged(MINUS)
    round_0(1)
    round_5(0)
    acts(2)
    round_6(0)
    round_1(1)
    acts(3)
    round_2(1)
    handed_own()
    handed(0, 1, 2, 3)
    near_tasks(0)
    round_3(1)
    acts(4)
    near_tasks(1)
    round_4(1)
    acts(5)
    handed(4, 5)
    for k in range(1, 8):
        to = lax.rem(t + k, 8)
        start(copy(opart.at[to], orecv.at[t], tsend, trecv, k - 1,
                   {"dp": dp, "tensor": to, "fsdp": y}))
    near_tasks(2)
    round_5(1)
    acts(6)
    handed(6)

    near_tasks(3)
    round_6(1, (6,))
    far_tasks(0, 2)
    round_6(1, (7, 8))
    far_tasks(2, 4)

    for k in range(1, 8):
        slot = orecv.at[mod(t - k, 8)]
        copy(slot, slot, tsend, trecv, k - 1, at_z(z, peer)).wait_recv()
    total = orecv[0]
    for k in range(1, 8):
        total += orecv[k]
    osum[...] = total
    klass = zh * 4 + zl
    train_share = copy(osum, otr, tsend, trecv, 7, at_z(z, peer))
    val_shares = []
    for zz in range(2):
        val_shares.append(copy(osum, ova, tsend, trecv, 8 + zz,
                               {"dp": zz * 4 + x, "tensor": klass, "fsdp": y}))
    own_val = [(c == 1) & (zh == zz) & (t == klass) for zz in range(2)]

    @pl.when(c == 0)
    def _():
        train_share.start()
        otr[...] = osum[...]

    for zz in range(2):
        @pl.when((c == 1) & jnp.logical_not(own_val[zz]))
        def _():
            val_shares[zz].start()

        @pl.when(own_val[zz])
        def _():
            ova[...] = osum[...]

    round_6(1, (9,))
    far_tasks(6, 1)

    def silu(v):
        return v / (1.0 + jnp.exp(-v))

    basis = ibasis[:, pl.ds(pl.multiple_of(zh * 640, 128), SPAN)]
    basis = jnp.concatenate([basis, basis], axis=0)
    hbuf[0 : SPAN - HALF] = jnp.zeros((SPAN - HALF, 256), BF16)
    hbuf[HALF:SPAN] = jnp.zeros((SPAN - HALF, 256), BF16)

    def project(half, n):
        tokens = pl.ds(pl.multiple_of(n * 256, 256), 256)
        hidden = silu(acc[half, 0:HALF, tokens]) * acc[half, HALF : 2 * HALF, tokens]
        hbuf[pl.ds(pl.multiple_of(zh * (SPAN - HALF), 16), HALF), :] = hidden.astype(BF16)
        value = jnp.dot(basis, hbuf[...], preferred_element_type=F32)
        proj[half, tokens, :] = value.T

    def last_task(n, carry):
        k = (1 - zh) * 4 + lax.rem(x + 2, 4)
        rows = jnp.concatenate([wf[k, i] for i in range(4)], axis=1)
        tokens = pl.ds(pl.multiple_of(n * 256, 256), 256)
        acc[1, :, tokens] += lax.dot_general(
            rows, xf[k, 1, n], (((1,), (1,)), ((), ())), preferred_element_type=F32)
        project(0, n)
        return carry

    lax.fori_loop(0, 2, last_task, 0)

    def last_half(n, carry):
        project(1, n)
        return carry

    lax.fori_loop(0, 2, last_half, 0)

    left = lax.broadcasted_iota(jnp.int32, (SEQ, 128), 1) < 64

    def message(zz, cc):
        train = proj[zz // 4, (zz % 4) * SEQ : (zz % 4 + 1) * SEQ, :]
        first = pl.multiple_of(256 + (2 * (zz % 2) + cc) * SEQ, SEQ)
        val = proj[(zz % 4) // 2, pl.ds(first, SEQ), :]
        return jnp.where(left, train, val)

    for zz in range(8):
        toward[zz] = message(zz, peer)
    start(copy(toward, given, tsend, trecv, 10, at_z(z, peer)))
    for zz in range(8):
        kept[zz] = message(zz, c)
    copy(given, given, tsend, trecv, 10, at_z(z, peer)).wait_recv()
    for zz in range(8):
        kept[zz] += given[zz]
    for k in range(1, 8):
        to = lax.rem(z + k, 8)
        start(copy(kept.at[to], irecv.at[z], tsend, trecv, 10 + k, at_z(to, c)))
    irecv[z] = kept[z]

    @pl.when(c == 1)
    def _():
        copy(otr, otr, tsend, trecv, 7, at_z(z, peer)).wait_recv()

    from_self = (zh == t // 4) & (t == lax.rem(t, 4) * 2 + 1)
    for zz in range(2):
        @pl.when((zh == zz) & jnp.logical_not(from_self))
        def _():
            copy(ova, ova, tsend, trecv, 8 + zz, at_z(z, peer)).wait_recv()

    for k in range(1, 8):
        slot = irecv.at[mod(z - k, 8)]
        copy(slot, slot, tsend, trecv, 10 + k, at_z(z, peer)).wait_recv()
    both = irecv[0]
    for k in range(1, 8):
        both += irecv[k]

    def unit(o_ref, first):
        sketch = lax.dot_general(
            both, o_ref[...], (((0,), (0,)), ((), ())),
            precision=lax.Precision.HIGHEST, preferred_element_type=F32)[first : first + 64]
        return sketch * lax.rsqrt(jnp.sum(sketch * sketch, keepdims=True) + 1e-06)

    vbuf[x * 4 + y] = unit(ova, 64).astype(BF16)
    n = 18
    for dx in range(4):
        for dy in range(4):
            if dx or dy:
                start(copy(vbuf.at[x * 4 + y], vbuf.at[x * 4 + y], tsend, trecv, n,
                           at_xy(lax.rem(x + dx, 4), lax.rem(y + dy, 4))))
                n += 1
    tbuf[zl] = unit(otr, 0)
    for k in range(1, 4):
        start(copy(tbuf.at[zl], tbuf.at[zl], tsend, trecv, 32 + k,
                   at_z(zh * 4 + lax.rem(zl + k, 4), c)))
    for k in range(1, 4):
        slot = tbuf.at[mod(zl - k, 4)]
        copy(slot, slot, tsend, trecv, 32 + k, at_z(z, peer)).wait_recv()
    n = 18
    for dx in range(4):
        for dy in range(4):
            if dx or dy:
                slot = vbuf.at[mod(x - dx, 4) * 4 + mod(y - dy, 4)]
                copy(slot, slot, tsend, trecv, n, at_z(z, peer)).wait_recv()
                n += 1

    where_r = lax.broadcasted_iota(jnp.int32, (16, 128), 0)
    where_l = lax.broadcasted_iota(jnp.int32, (16, 128), 1)
    place = where_l == where_r * 4 + (t // 4) * 64 + lax.rem(t, 4)
    vals = [vbuf[v].astype(F32) for v in range(16)]
    lines = []
    for i in range(4):
        train = tbuf[i]
        pairs = jnp.concatenate(
            [jnp.sum(train * val, axis=0, keepdims=True) for val in vals], axis=0)
        dots = jnp.sum(pairs, axis=1, keepdims=True) * jnp.sqrt(jnp.float32(64 * 128))
        lines.append(jnp.sum(jnp.where(place, dots, 0.0), axis=0, keepdims=True))
    row[...] = jnp.concatenate(lines + [jnp.zeros((4, 128), F32)], axis=0)
    for k in range(1, 8):
        to = lax.rem(t + k, 8)
        start(copy(row, obuf.at[t], tsend, trecv, 35 + k, {"dp": dp, "tensor": to, "fsdp": y}))
    obuf[t] = row[...]
    for k in range(1, 8):
        slot = obuf.at[mod(t - k, 8)]
        copy(slot, slot, tsend, trecv, 35 + k, at_z(z, peer)).wait_recv()
    scores = obuf[0]
    for k in range(1, 8):
        scores += obuf[k]
    out[...] = scores[0:4]

    for c_ in started:
        c_.wait_send()

    @pl.when(c == 0)
    def _():
        train_share.wait_send()

    for zz in range(2):
        @pl.when((c == 1) & jnp.logical_not(own_val[zz]))
        def _():
            val_shares[zz].wait_send()


def on_device(
    train_acts, val_acts, train_cot, val_cot, train_lengths, val_lengths,
    gate_weight, up_weight, in_basis, out_basis,
):
    vmem = pl.BlockSpec(memory_space=pltpu.VMEM)
    dma = pltpu.SemaphoreType.DMA
    return pl.pallas_call(
        body,
        out_shape=jax.ShapeDtypeStruct((4, 128), F32),
        in_specs=[pl.BlockSpec(memory_space=pl.ANY)] * 10,
        out_specs=vmem,
        scratch_shapes=[
            pltpu.SMEM((4,), jnp.int32),
            pltpu.SMEM((4,), jnp.int32),
            pltpu.VMEM((2, HALF, 128), BF16),
            pltpu.VMEM((2, 256, 512), BF16),
            pltpu.VMEM((64, 1376), BF16),
            pltpu.VMEM((512, 128), BF16),
            pltpu.VMEM((8, 4, 2 * HALF, 128), BF16),
            pltpu.VMEM((2, HALF, 128), BF16),
            pltpu.VMEM((8, 2, 2, 256, 512), BF16),
            pltpu.VMEM((2, 2 * HALF, 512), F32),
            pltpu.VMEM((SPAN, 256), BF16),
            pltpu.VMEM((2, 512, 128), F32),
            pltpu.VMEM((8, SEQ, 128), F32),
            pltpu.VMEM((8, SEQ, 128), F32),
            pltpu.VMEM((SEQ, 128), F32),
            pltpu.VMEM((SEQ, 128), F32),
            pltpu.VMEM((SEQ, 128), F32),
            pltpu.VMEM((8, SEQ, 128), F32),
            pltpu.VMEM((8, SEQ, 128), F32),
            pltpu.VMEM((8, SEQ, 128), F32),
            pltpu.VMEM((8, SEQ, 128), F32),
            pltpu.VMEM((4, 64, 128), F32),
            pltpu.VMEM((16, 64, 128), BF16),
            pltpu.VMEM((8, 128), F32),
            pltpu.VMEM((8, 8, 128), F32),
            dma((80,)), dma((80,)),
            dma((18,)), dma((18,)),
            dma((16,)), dma((16,)),
            dma((43,)), dma((43,)),
            dma((12,)),
        ],
        compiler_params=pltpu.CompilerParams(
            collective_id=0, has_side_effects=True, vmem_limit_bytes=60 * 1024 * 1024
        ),
    )(train_lengths, val_lengths, gate_weight.T, up_weight.T, train_acts, val_acts,
      train_cot, val_cot, in_basis.T, out_basis)


def solution(mesh):
    rows = P(("dp", "fsdp"), "tensor")
    placed = (rows, rows, rows, rows, P(("dp", "fsdp")), P(("dp", "fsdp")), rows, rows,
              P("tensor", None), P("tensor", None))
    return jax.shard_map(
        on_device, mesh=mesh, in_specs=placed, out_specs=P(("dp", "fsdp"), None), check_vma=False
    )
```

```python
import jax
import jax.numpy as jnp
from jax import lax
from jax.experimental import pallas as pl
from jax.experimental.pallas import tpu as pltpu
from jax.sharding import PartitionSpec as P

SEQ = 64
MESH = pl.DeviceIdType.MESH
F32 = jnp.float32
BF16 = jnp.bfloat16
HALF = 688
SPAN = 736
CUT = 352
PLUS, MINUS = 1, -1


def mod(value, n):
    return lax.rem(value + n, n)


def body(
    tlen_in, vlen_in, gate, up, tacts, vacts, tcot, vcot, ibasis_in, obasis_in,
    out,
    tlen, vlen, other, cots, ibasis, obasis, wf, relay, xf, acc, hbuf, proj, opart, orecv, osum, otr, ova,
    toward, kept, given, passed, irecv, tbuf, vbuf, row, obuf,
    wsend, wrecv, zsend, zrecv, dsend, drecv, tsend, trecv, isem,
):
    dp = lax.axis_index("dp")
    t = lax.axis_index("tensor")
    y = lax.axis_index("fsdp")
    zh = dp // 4
    x = lax.rem(dp, 4)
    zl = t // 2
    c = lax.rem(t, 2)
    z = zh * 4 + zl
    peer = 1 - c

    def at_z(zz, cc):
        return {"dp": (zz // 4) * 4 + x, "tensor": lax.rem(zz, 4) * 2 + cc, "fsdp": y}

    def at_xy(xx, yy):
        return {"dp": zh * 4 + xx, "tensor": t, "fsdp": yy}

    def copy(src, dst, sends, recvs, n, device):
        return pltpu.make_async_remote_copy(
            src_ref=src, dst_ref=dst, send_sem=sends.at[n], recv_sem=recvs.at[n],
            device_id=device, device_id_type=MESH,
        )

    started = []

    def start(c_):
        c_.start()
        started.append(c_)

    barrier = pltpu.get_barrier_semaphore()
    near = [at_xy(mod(x + s, 4), y) for s in (1, -1)] + [at_xy(x, mod(y + s, 4)) for s in (1, -1)]
    near += [at_z(mod(z + s, 8), c) for s in (1, -1, 2, -2)] + [at_z(z, peer)]
    for device in near:
        pl.semaphore_signal(barrier, inc=1, device_id=device, device_id_type=MESH)

    def own_rows(half):
        return pl.ds(pl.multiple_of(half * HALF, 16), HALF)

    fetches = [
        (gate.at[own_rows(zh), :], wf.at[dp, y, pl.ds(0, HALF), :]),
        (up.at[own_rows(zh), :], wf.at[dp, y, pl.ds(HALF, HALF), :]),
        (gate.at[own_rows(1 - zh), :], other.at[0]), (up.at[own_rows(1 - zh), :], other.at[1]),
        (tacts, xf.at[t, zh, 0]), (vacts, xf.at[t, zh, 1]),
        (tcot, cots.at[0]), (vcot, cots.at[1]), (obasis_in, obasis), (ibasis_in, ibasis),
        (tlen_in, tlen), (vlen_in, vlen),
    ]
    fetches = [pltpu.make_async_copy(a, b, isem.at[n]) for n, (a, b) in enumerate(fetches)]
    for fetch in fetches:
        fetch.start()
    for fetch in fetches[:6]:
        fetch.wait()
    pl.semaphore_wait(barrier, len(near))

    def w_rows(zc, xx, yy, part, half=None):
        first, count = {None: (0, HALF), 0: (0, CUT), 1: (CUT, HALF - CUT)}[half]
        return wf.at[zc * 4 + xx, yy, pl.ds(part * HALF + first, count), :]

    def exchange(sign):
        n = 0 if sign == PLUS else 1
        start(copy(other.at[n], relay.at[n], zsend, zrecv, n,
                   at_z(mod(z + 2 * sign, 8), c)))

    def exchange_on(sign):
        n = 0 if sign == PLUS else 1
        copy(relay.at[n], relay.at[n], zsend, zrecv, n, at_z(z, peer)).wait_recv()
        origin = mod(z - 2 * sign, 8)
        slot = w_rows(origin // 4, x, y, n)
        start(copy(relay.at[n], slot, zsend, zrecv, 2 + n, at_z(mod(z + 2 * sign, 8), c)))

    def exchanged(sign):
        n = 0 if sign == PLUS else 1
        slot = w_rows(1 - zh, x, y, n)
        copy(slot, slot, zsend, zrecv, 2 + n, at_z(z, peer)).wait_recv()

    def act_slot(zz, cc, kind):
        return xf.at[lax.rem(zz, 4) * 2 + cc, zz // 4, kind]

    def kind_of(sign, n):
        return n % 2 if sign == PLUS else 1 - n % 2

    def act_send(sign, n):
        kind = kind_of(sign, n)
        base = 4 if sign == PLUS else 11
        slot = act_slot(mod(z - sign * (n // 2), 8), c, kind)
        start(copy(slot, slot, zsend, zrecv, base + n, at_z(mod(z + sign, 8), c)))

    def hand_over(slot, n):
        start(copy(slot, slot, dsend, drecv, n, at_z(z, peer)))

    def act_arrive(sign, n):
        base = 4 if sign == PLUS else 11
        slot = act_slot(mod(z - sign * (n // 2 + 1), 8), c, kind_of(sign, n))
        copy(slot, slot, zsend, zrecv, base + n, at_z(z, peer)).wait_recv()
        if n + 2 < 7:
            act_send(sign, n + 2)
        hand_over(slot, 2 + (n if sign == PLUS else 7 + n))

    def handed_own():
        for kind in range(2):
            slot = act_slot(z, peer, kind)
            copy(slot, slot, dsend, drecv, kind, at_z(z, peer)).wait_recv()

    def handed(*steps):
        for n in steps:
            for sign in (PLUS, MINUS):
                slot = act_slot(mod(z - sign * (n // 2 + 1), 8), peer, kind_of(sign, n))
                copy(slot, slot, dsend, drecv, 2 + (n if sign == PLUS else 7 + n),
                     at_z(z, peer)).wait_recv()

    def acts(n):
        for sign in (PLUS, MINUS):
            act_arrive(sign, n)

    def w_part(cls, axis, da, db, part, half):
        xx, yy = (mod(x + da, 4), mod(y + db, 4)) if axis == 0 else (mod(x + db, 4), mod(y + da, 4))
        zc = zh if cls == 0 else 1 - zh
        return w_rows(zc, xx, yy, part, half)

    def w_where(cls, axis, sign, name, shift):
        first, second = axis, 1 - axis
        half = 0 if sign == PLUS else 1
        da, db, part, cut = {
            0: (0, 0, first, None), 1: (0, 0, second, None), 2: (-sign, 0, first, half),
            3: (0, -1, second, None), 4: (0, 1, second, None), 5: (0, 2, second, None),
            6: (-sign, 0, second, half), 7: (-sign, -1, second, half),
            8: (-sign, 1, second, half), 9: (-sign, 2, second, half),
        }[name]
        return w_part(cls, axis, da - shift * sign, db, part, cut)

    def w_id(cls, axis, sign, name):
        return ((cls * 2 + axis) * 2 + (0 if sign == PLUS else 1)) * 10 + name

    def w_send(cls, axis, sign, name):
        ref = w_where(cls, axis, sign, name, 0)
        to = at_xy(mod(x + sign, 4), y) if axis == 0 else at_xy(x, mod(y + sign, 4))
        start(copy(ref, ref, wsend, wrecv, w_id(cls, axis, sign, name), to))

    def w_arrive(cls, axis, sign, name):
        ref = w_where(cls, axis, sign, name, 1)
        copy(ref, ref, wsend, wrecv, w_id(cls, axis, sign, name), at_z(z, peer)).wait_recv()

    ways = [(axis, sign) for axis in (0, 1) for sign in (PLUS, MINUS)]

    def round_0(cls):
        for name in (0, 1):
            for axis, sign in ways:
                w_send(cls, axis, sign, name)

    def round_1(cls):
        for axis, sign in ways:
            w_arrive(cls, axis, sign, 0)
            w_send(cls, axis, sign, 2)
            for other in (PLUS, MINUS):
                w_send(cls, 1 - axis, other, 3 if sign == PLUS else 4)

    def round_2(cls):
        for axis, sign in ways:
            w_arrive(cls, axis, sign, 1)
            w_send(cls, axis, sign, 6)

    def round_3(cls):
        for axis in (0, 1):
            w_arrive(cls, axis, PLUS, 2)
            w_arrive(cls, axis, MINUS, 2)
            for other in (PLUS, MINUS):
                w_send(cls, 1 - axis, other, 5)

    def round_4(cls):
        for name in (3, 4):
            for axis, sign in ways:
                w_arrive(cls, axis, sign, name)
                w_send(cls, axis, sign, name + 4)

    def round_5(cls):
        for axis, sign in ways:
            w_arrive(cls, axis, sign, 5)
            w_send(cls, axis, sign, 9)

    def round_6(cls, names=(6, 7, 8, 9)):
        for name in names:
            for axis, sign in ways:
                w_arrive(cls, axis, sign, name)

    def multiply(half, k):
        rows = jnp.concatenate([wf[k, i] for i in range(4)], axis=1)
        acc[half] += lax.dot_general(
            rows, xf[k, half].reshape(512, 512), (((1,), (1,)), ((), ())),
            preferred_element_type=F32)

    away = []
    for m in range(4):
        there = (m // 2) * 4 + 2 * zh + m % 2
        ahead = mod(there - z, 8)
        away.append(jnp.minimum(ahead, lax.rem(8 - ahead, 8)) * 4 + m)
    nearest = []
    for p in range(4):
        pick = 0
        for m in range(4):
            rank = sum((away[o] < away[m]).astype(jnp.int32) for o in range(4) if o != m)
            pick = pick + m * (rank == p).astype(jnp.int32)
        nearest.append(pick)

    def near_tasks(p):
        def step(n, carry):
            multiply(nearest[p] // 2, zh * 4 + 2 * lax.rem(nearest[p], 2) + n)
            return carry

        lax.fori_loop(0, 2, step, 0)

    def far_tasks(first, count):
        def step(n, carry):
            g = n // 2
            dx = g + (g == 2).astype(jnp.int32) - (g == 3).astype(jnp.int32)
            multiply(lax.rem(n, 2), (1 - zh) * 4 + lax.rem(x + dx, 4))
            return carry

        lax.fori_loop(first, first + count, step, 0)

    def gap(half):
        ahead = mod(half * 4 + 2 * (1 - zh) + x // 2 - z, 8)
        return jnp.minimum(ahead, lax.rem(8 - ahead, 8))

    nearer = (gap(1) < gap(0)).astype(jnp.int32)

    exchange(PLUS)
    exchange(MINUS)
    round_0(0)
    act_send(PLUS, 0)
    act_send(MINUS, 0)
    hand_over(act_slot(z, c, 0), 0)
    hand_over(act_slot(z, c, 1), 1)
    acc[...] = jnp.zeros_like(acc)

    for fetch in fetches[6:]:
        fetch.wait()
    slots = lax.broadcasted_iota(jnp.int32, (SEQ, 128), 0)
    for kind, lens in enumerate((tlen, vlen)):
        value = jnp.dot(cots[kind], obasis[...], preferred_element_type=F32)
        for i in range(4):
            rows = value[i * SEQ : (i + 1) * SEQ]
            opart[2 * i + kind] = jnp.where(slots < lens[i], rows, 0.0)
    orecv[t] = opart[t]

    round_1(0)
    round_2(0)
    exchange_on(PLUS)
    exchange_on(MINUS)
    act_send(PLUS, 1)
    act_send(MINUS, 1)
    round_3(0)
    acts(0)
    round_4(0)
    exchanged(PLUS)
    exchanged(MINUS)
    round_0(1)
    acts(1)
    round_5(0)
    acts(2)
    round_1(1)
    acts(3)
    round_6(0)
    round_2(1)
    handed_own()
    handed(0, 1, 2, 3)
    near_tasks(0)
    round_3(1)
    acts(4)
    near_tasks(1)
    round_4(1)
    for sign in (PLUS, MINUS):
        w_arrive(1, 1, sign, 6)
    multiply(nearer, (1 - zh) * 4 + x)
    acts(5)
    handed(4, 5)
    near_tasks(2)
    round_5(1)
    acts(6)
    handed(6)
    for k in range(1, 8):
        to = lax.rem(t + k, 8)
        start(copy(opart.at[to], orecv.at[t], tsend, trecv, k - 1,
                   {"dp": dp, "tensor": to, "fsdp": y}))

    near_tasks(3)
    multiply(1 - nearer, (1 - zh) * 4 + x)
    for sign in (PLUS, MINUS):
        w_arrive(1, 0, sign, 6)
    round_6(1, (7, 8))
    far_tasks(2, 4)

    round_6(1, (9,))
    far_tasks(6, 1)

    for k in range(1, 8):
        slot = orecv.at[mod(t - k, 8)]
        copy(slot, slot, tsend, trecv, k - 1, at_z(z, peer)).wait_recv()
    total = orecv[0]
    for k in range(1, 8):
        total += orecv[k]
    osum[...] = total
    klass = zh * 4 + zl
    train_share = copy(osum, otr, tsend, trecv, 7, at_z(z, peer))
    val_shares = []
    for zz in range(2):
        val_shares.append(copy(osum, ova, tsend, trecv, 8 + zz,
                               {"dp": zz * 4 + x, "tensor": klass, "fsdp": y}))
    own_val = [(c == 1) & (zh == zz) & (t == klass) for zz in range(2)]

    @pl.when(c == 0)
    def _():
        train_share.start()
        otr[...] = osum[...]

    for zz in range(2):
        @pl.when((c == 1) & jnp.logical_not(own_val[zz]))
        def _():
            val_shares[zz].start()

        @pl.when(own_val[zz])
        def _():
            ova[...] = osum[...]

    def silu(v):
        return v / (1.0 + jnp.exp(-v))

    basis = ibasis[:, pl.ds(pl.multiple_of(zh * 640, 128), SPAN)]
    basis = jnp.concatenate([basis, basis], axis=0)
    hbuf[0 : SPAN - HALF] = jnp.zeros((SPAN - HALF, 256), BF16)
    hbuf[HALF:SPAN] = jnp.zeros((SPAN - HALF, 256), BF16)

    def project(half, n):
        tokens = pl.ds(pl.multiple_of(n * 256, 256), 256)
        hidden = silu(acc[half, 0:HALF, tokens]) * acc[half, HALF : 2 * HALF, tokens]
        hbuf[pl.ds(pl.multiple_of(zh * (SPAN - HALF), 16), HALF), :] = hidden.astype(BF16)
        value = jnp.dot(basis, hbuf[...], preferred_element_type=F32)
        proj[half, tokens, :] = value.T

    def last_task(n, carry):
        k = (1 - zh) * 4 + lax.rem(x + 2, 4)
        rows = jnp.concatenate([wf[k, i] for i in range(4)], axis=1)
        tokens = pl.ds(pl.multiple_of(n * 256, 256), 256)
        acc[1, :, tokens] += lax.dot_general(
            rows, xf[k, 1, n], (((1,), (1,)), ((), ())), preferred_element_type=F32)
        project(0, n)
        return carry

    lax.fori_loop(0, 2, last_task, 0)

    def last_half(n, carry):
        project(1, n)
        return carry

    lax.fori_loop(0, 2, last_half, 0)

    left = lax.broadcasted_iota(jnp.int32, (SEQ, 128), 1) < 64

    def message(zz, cc):
        train = proj[zz // 4, (zz % 4) * SEQ : (zz % 4 + 1) * SEQ, :]
        first = pl.multiple_of(256 + (2 * (zz % 2) + cc) * SEQ, SEQ)
        val = proj[(zz % 4) // 2, pl.ds(first, SEQ), :]
        return jnp.where(left, train, val)

    for zz in range(8):
        toward[zz] = message(zz, peer)
    start(copy(toward, given, tsend, trecv, 10, at_z(z, peer)))
    for zz in range(8):
        kept[zz] = message(zz, c)
    copy(given, given, tsend, trecv, 10, at_z(z, peer)).wait_recv()
    for zz in range(8):
        passed[zz] = (kept[zz] + given[zz]).astype(BF16)
    for k in range(1, 8):
        to = lax.rem(z + k, 8)
        start(copy(passed.at[to], irecv.at[z], tsend, trecv, 10 + k, at_z(to, c)))
    both = kept[z] + given[z]

    @pl.when(c == 1)
    def _():
        copy(otr, otr, tsend, trecv, 7, at_z(z, peer)).wait_recv()

    from_self = (zh == t // 4) & (t == lax.rem(t, 4) * 2 + 1)
    for zz in range(2):
        @pl.when((zh == zz) & jnp.logical_not(from_self))
        def _():
            copy(ova, ova, tsend, trecv, 8 + zz, at_z(z, peer)).wait_recv()

    for k in range(1, 8):
        slot = irecv.at[mod(z - k, 8)]
        copy(slot, slot, tsend, trecv, 10 + k, at_z(z, peer)).wait_recv()
    for k in range(1, 8):
        both += irecv[mod(z - k, 8)].astype(F32)

    def unit(o_ref, first):
        sketch = lax.dot_general(
            both, o_ref[...], (((0,), (0,)), ((), ())),
            precision=lax.Precision.HIGHEST, preferred_element_type=F32)[first : first + 64]
        return sketch * lax.rsqrt(jnp.sum(sketch * sketch, keepdims=True) + 1e-06)

    vbuf[x * 4 + y] = unit(ova, 64).astype(BF16)
    n = 18
    for dx in range(4):
        for dy in range(4):
            if dx or dy:
                start(copy(vbuf.at[x * 4 + y], vbuf.at[x * 4 + y], tsend, trecv, n,
                           at_xy(lax.rem(x + dx, 4), lax.rem(y + dy, 4))))
                n += 1
    tbuf[zl] = unit(otr, 0)
    for k in range(1, 4):
        start(copy(tbuf.at[zl], tbuf.at[zl], tsend, trecv, 32 + k,
                   at_z(zh * 4 + lax.rem(zl + k, 4), c)))
    for k in range(1, 4):
        slot = tbuf.at[mod(zl - k, 4)]
        copy(slot, slot, tsend, trecv, 32 + k, at_z(z, peer)).wait_recv()
    n = 18
    for dx in range(4):
        for dy in range(4):
            if dx or dy:
                slot = vbuf.at[mod(x - dx, 4) * 4 + mod(y - dy, 4)]
                copy(slot, slot, tsend, trecv, n, at_z(z, peer)).wait_recv()
                n += 1

    where_r = lax.broadcasted_iota(jnp.int32, (128, 128), 0)
    where_l = lax.broadcasted_iota(jnp.int32, (128, 128), 1)
    place = where_l == (where_r // 8) * 4 + (t // 4) * 64 + lax.rem(t, 4)
    blocks = [[] for _ in range(4)]
    for v in range(16):
        val = vbuf[v].astype(F32)
        for i in range(4):
            product = tbuf[i] * val
            parts = [product[8 * q : 8 * q + 8] for q in range(8)]
            while len(parts) > 1:
                parts = [parts[q] + parts[q + 1] for q in range(0, len(parts), 2)]
            blocks[i].append(parts[0])
    lines = []
    for i in range(4):
        dots = jnp.sum(jnp.concatenate(blocks[i], axis=0), axis=1, keepdims=True)
        dots = dots * jnp.sqrt(jnp.float32(64 * 128))
        lines.append(jnp.sum(jnp.where(place, dots, 0.0), axis=0, keepdims=True))
    row[...] = jnp.concatenate(lines + [jnp.zeros((4, 128), F32)], axis=0)
    for k in range(1, 8):
        to = lax.rem(t + k, 8)
        start(copy(row, obuf.at[t], tsend, trecv, 35 + k, {"dp": dp, "tensor": to, "fsdp": y}))
    obuf[t] = row[...]
    for k in range(1, 8):
        slot = obuf.at[mod(t - k, 8)]
        copy(slot, slot, tsend, trecv, 35 + k, at_z(z, peer)).wait_recv()
    scores = obuf[0]
    for k in range(1, 8):
        scores += obuf[k]
    out[...] = scores[0:4]

    for c_ in started:
        c_.wait_send()

    @pl.when(c == 0)
    def _():
        train_share.wait_send()

    for zz in range(2):
        @pl.when((c == 1) & jnp.logical_not(own_val[zz]))
        def _():
            val_shares[zz].wait_send()


def on_device(
    train_acts, val_acts, train_cot, val_cot, train_lengths, val_lengths,
    gate_weight, up_weight, in_basis, out_basis,
):
    vmem = pl.BlockSpec(memory_space=pltpu.VMEM)
    dma = pltpu.SemaphoreType.DMA
    return pl.pallas_call(
        body,
        out_shape=jax.ShapeDtypeStruct((4, 128), F32),
        in_specs=[pl.BlockSpec(memory_space=pl.ANY)] * 10,
        out_specs=vmem,
        scratch_shapes=[
            pltpu.SMEM((4,), jnp.int32),
            pltpu.SMEM((4,), jnp.int32),
            pltpu.VMEM((2, HALF, 128), BF16),
            pltpu.VMEM((2, 256, 512), BF16),
            pltpu.VMEM((64, 1376), BF16),
            pltpu.VMEM((512, 128), BF16),
            pltpu.VMEM((8, 4, 2 * HALF, 128), BF16),
            pltpu.VMEM((2, HALF, 128), BF16),
            pltpu.VMEM((8, 2, 2, 256, 512), BF16),
            pltpu.VMEM((2, 2 * HALF, 512), F32),
            pltpu.VMEM((SPAN, 256), BF16),
            pltpu.VMEM((2, 512, 128), F32),
            pltpu.VMEM((8, SEQ, 128), F32),
            pltpu.VMEM((8, SEQ, 128), F32),
            pltpu.VMEM((SEQ, 128), F32),
            pltpu.VMEM((SEQ, 128), F32),
            pltpu.VMEM((SEQ, 128), F32),
            pltpu.VMEM((8, SEQ, 128), F32),
            pltpu.VMEM((8, SEQ, 128), F32),
            pltpu.VMEM((8, SEQ, 128), F32),
            pltpu.VMEM((8, SEQ, 128), BF16),
            pltpu.VMEM((8, SEQ, 128), BF16),
            pltpu.VMEM((4, 64, 128), F32),
            pltpu.VMEM((16, 64, 128), BF16),
            pltpu.VMEM((8, 128), F32),
            pltpu.VMEM((8, 8, 128), F32),
            dma((80,)), dma((80,)),
            dma((18,)), dma((18,)),
            dma((16,)), dma((16,)),
            dma((43,)), dma((43,)),
            dma((12,)),
        ],
        compiler_params=pltpu.CompilerParams(
            collective_id=0, has_side_effects=True, vmem_limit_bytes=60 * 1024 * 1024
        ),
    )(train_lengths, val_lengths, gate_weight.T, up_weight.T, train_acts, val_acts,
      train_cot, val_cot, in_basis.T, out_basis)


def solution(mesh):
    rows = P(("dp", "fsdp"), "tensor")
    placed = (rows, rows, rows, rows, P(("dp", "fsdp")), P(("dp", "fsdp")), rows, rows,
              P("tensor", None), P("tensor", None))
    return jax.shard_map(
        on_device, mesh=mesh, in_specs=placed, out_specs=P(("dp", "fsdp"), None), check_vma=False
    )
```

```python
import jax
import jax.numpy as jnp
from jax import lax
from jax.experimental import pallas as pl
from jax.experimental.pallas import tpu as pltpu
from jax.sharding import PartitionSpec as P

SEQ = 64
MESH = pl.DeviceIdType.MESH
F32 = jnp.float32
BF16 = jnp.bfloat16
HALF = 688
SPAN = 736
CUT = 352
PLUS, MINUS = 1, -1


def mod(value, n):
    return lax.rem(value + n, n)


def body(
    tlen_in, vlen_in, gate, up, tacts, vacts, tcot, vcot, ibasis_in, obasis_in,
    out,
    tlen, vlen, other, cots, ibasis, obasis, wf, relay, xf, acc, hbuf, proj, opart, orecv, osum, otr, ova,
    toward, kept, given, passed, irecv, tbuf, vbuf, row, obuf,
    wsend, wrecv, zsend, zrecv, dsend, drecv, tsend, trecv, isem,
):
    dp = lax.axis_index("dp")
    t = lax.axis_index("tensor")
    y = lax.axis_index("fsdp")
    zh = dp // 4
    x = lax.rem(dp, 4)
    zl = t // 2
    c = lax.rem(t, 2)
    z = zh * 4 + zl
    peer = 1 - c

    def at_z(zz, cc):
        return {"dp": (zz // 4) * 4 + x, "tensor": lax.rem(zz, 4) * 2 + cc, "fsdp": y}

    def at_xy(xx, yy):
        return {"dp": zh * 4 + xx, "tensor": t, "fsdp": yy}

    def copy(src, dst, sends, recvs, n, device):
        return pltpu.make_async_remote_copy(
            src_ref=src, dst_ref=dst, send_sem=sends.at[n], recv_sem=recvs.at[n],
            device_id=device, device_id_type=MESH,
        )

    started = []

    def start(c_):
        c_.start()
        started.append(c_)

    barrier = pltpu.get_barrier_semaphore()
    near = [at_xy(mod(x + s, 4), y) for s in (1, -1)] + [at_xy(x, mod(y + s, 4)) for s in (1, -1)]
    near += [at_z(mod(z + s, 8), c) for s in (1, -1, 2, -2)] + [at_z(z, peer)]
    for device in near:
        pl.semaphore_signal(barrier, inc=1, device_id=device, device_id_type=MESH)

    def own_rows(half):
        return pl.ds(pl.multiple_of(half * HALF, 16), HALF)

    fetches = [
        (gate.at[own_rows(zh), :], wf.at[dp, y, pl.ds(0, HALF), :]),
        (up.at[own_rows(zh), :], wf.at[dp, y, pl.ds(HALF, HALF), :]),
        (gate.at[own_rows(1 - zh), :], other.at[0]), (up.at[own_rows(1 - zh), :], other.at[1]),
        (tacts, xf.at[t, zh, 0]), (vacts, xf.at[t, zh, 1]),
        (tcot, cots.at[0]), (vcot, cots.at[1]), (obasis_in, obasis), (ibasis_in, ibasis),
        (tlen_in, tlen), (vlen_in, vlen),
    ]
    fetches = [pltpu.make_async_copy(a, b, isem.at[n]) for n, (a, b) in enumerate(fetches)]
    for fetch in fetches:
        fetch.start()
    for fetch in fetches[:6]:
        fetch.wait()
    pl.semaphore_wait(barrier, len(near))

    def w_rows(zc, xx, yy, part, half=None):
        first, count = {None: (0, HALF), 0: (0, CUT), 1: (CUT, HALF - CUT)}[half]
        return wf.at[zc * 4 + xx, yy, pl.ds(part * HALF + first, count), :]

    def exchange(sign):
        n = 0 if sign == PLUS else 1
        start(copy(other.at[n], relay.at[n], zsend, zrecv, n,
                   at_z(mod(z + 2 * sign, 8), c)))

    def exchange_on(sign):
        n = 0 if sign == PLUS else 1
        copy(relay.at[n], relay.at[n], zsend, zrecv, n, at_z(z, peer)).wait_recv()
        origin = mod(z - 2 * sign, 8)
        slot = w_rows(origin // 4, x, y, n)
        start(copy(relay.at[n], slot, zsend, zrecv, 2 + n, at_z(mod(z + 2 * sign, 8), c)))

    def exchanged(sign):
        n = 0 if sign == PLUS else 1
        slot = w_rows(1 - zh, x, y, n)
        copy(slot, slot, zsend, zrecv, 2 + n, at_z(z, peer)).wait_recv()

    def act_slot(zz, cc, kind):
        return xf.at[lax.rem(zz, 4) * 2 + cc, zz // 4, kind]

    def kind_of(sign, n):
        return n % 2 if sign == PLUS else 1 - n % 2

    def act_send(sign, n):
        kind = kind_of(sign, n)
        base = 4 if sign == PLUS else 11
        slot = act_slot(mod(z - sign * (n // 2), 8), c, kind)
        start(copy(slot, slot, zsend, zrecv, base + n, at_z(mod(z + sign, 8), c)))

    def hand_over(slot, n):
        start(copy(slot, slot, dsend, drecv, n, at_z(z, peer)))

    def act_arrive(sign, n):
        base = 4 if sign == PLUS else 11
        slot = act_slot(mod(z - sign * (n // 2 + 1), 8), c, kind_of(sign, n))
        copy(slot, slot, zsend, zrecv, base + n, at_z(z, peer)).wait_recv()
        if n + 2 < 7:
            act_send(sign, n + 2)
        hand_over(slot, 2 + (n if sign == PLUS else 7 + n))

    def handed_own():
        for kind in range(2):
            slot = act_slot(z, peer, kind)
            copy(slot, slot, dsend, drecv, kind, at_z(z, peer)).wait_recv()

    def handed(*steps):
        for n in steps:
            for sign in (PLUS, MINUS):
                slot = act_slot(mod(z - sign * (n // 2 + 1), 8), peer, kind_of(sign, n))
                copy(slot, slot, dsend, drecv, 2 + (n if sign == PLUS else 7 + n),
                     at_z(z, peer)).wait_recv()

    def acts(n):
        for sign in (PLUS, MINUS):
            act_arrive(sign, n)

    def w_part(cls, axis, da, db, part, half):
        xx, yy = (mod(x + da, 4), mod(y + db, 4)) if axis == 0 else (mod(x + db, 4), mod(y + da, 4))
        zc = zh if cls == 0 else 1 - zh
        return w_rows(zc, xx, yy, part, half)

    def w_where(cls, axis, sign, name, shift):
        first, second = axis, 1 - axis
        half = 0 if sign == PLUS else 1
        da, db, part, cut = {
            0: (0, 0, first, None), 1: (0, 0, second, None), 2: (-sign, 0, first, half),
            3: (0, -1, second, None), 4: (0, 1, second, None), 5: (0, 2, second, None),
            6: (-sign, 0, second, half), 7: (-sign, -1, second, half),
            8: (-sign, 1, second, half), 9: (-sign, 2, second, half),
        }[name]
        return w_part(cls, axis, da - shift * sign, db, part, cut)

    def w_id(cls, axis, sign, name):
        return ((cls * 2 + axis) * 2 + (0 if sign == PLUS else 1)) * 10 + name

    def w_send(cls, axis, sign, name):
        ref = w_where(cls, axis, sign, name, 0)
        to = at_xy(mod(x + sign, 4), y) if axis == 0 else at_xy(x, mod(y + sign, 4))
        start(copy(ref, ref, wsend, wrecv, w_id(cls, axis, sign, name), to))

    def w_arrive(cls, axis, sign, name):
        ref = w_where(cls, axis, sign, name, 1)
        copy(ref, ref, wsend, wrecv, w_id(cls, axis, sign, name), at_z(z, peer)).wait_recv()

    ways = [(axis, sign) for axis in (0, 1) for sign in (PLUS, MINUS)]

    def round_0(cls):
        for name in (0, 1):
            for axis, sign in ways:
                w_send(cls, axis, sign, name)

    def round_1(cls):
        for axis, sign in ways:
            w_arrive(cls, axis, sign, 0)
            w_send(cls, axis, sign, 2)
            for other in (PLUS, MINUS):
                w_send(cls, 1 - axis, other, 3 if sign == PLUS else 4)

    def round_2(cls):
        for axis, sign in ways:
            w_arrive(cls, axis, sign, 1)
            w_send(cls, axis, sign, 6)

    def round_3(cls):
        for axis in (0, 1):
            w_arrive(cls, axis, PLUS, 2)
            w_arrive(cls, axis, MINUS, 2)
            for other in (PLUS, MINUS):
                w_send(cls, 1 - axis, other, 5)

    def round_4(cls):
        for name in (3, 4):
            for axis, sign in ways:
                w_arrive(cls, axis, sign, name)
                w_send(cls, axis, sign, name + 4)

    def round_5(cls):
        for axis, sign in ways:
            w_arrive(cls, axis, sign, 5)
            w_send(cls, axis, sign, 9)

    def round_6(cls, names=(6, 7, 8, 9)):
        for name in names:
            for axis, sign in ways:
                w_arrive(cls, axis, sign, name)

    def multiply(half, *ks):
        rows = jnp.concatenate([wf[k, i] for k in ks for i in range(4)], axis=1)
        tokens = jnp.concatenate([xf[k, half].reshape(512, 512) for k in ks], axis=1)
        acc[half] += lax.dot_general(
            rows, tokens, (((1,), (1,)), ((), ())), preferred_element_type=F32)

    away = []
    for m in range(4):
        there = (m // 2) * 4 + 2 * zh + m % 2
        ahead = mod(there - z, 8)
        away.append(jnp.minimum(ahead, lax.rem(8 - ahead, 8)) * 4 + m)
    nearest = []
    for p in range(4):
        pick = 0
        for m in range(4):
            rank = sum((away[o] < away[m]).astype(jnp.int32) for o in range(4) if o != m)
            pick = pick + m * (rank == p).astype(jnp.int32)
        nearest.append(pick)

    def near_tasks(p):
        first = zh * 4 + 2 * lax.rem(nearest[p], 2)
        multiply(nearest[p] // 2, first, first + 1)

    def side_tasks():
        def step(half, carry):
            multiply(half, (1 - zh) * 4 + lax.rem(x + 1, 4), (1 - zh) * 4 + lax.rem(x + 3, 4))
            return carry

        lax.fori_loop(0, 2, step, 0)

    def gap(half):
        ahead = mod(half * 4 + 2 * (1 - zh) + x // 2 - z, 8)
        return jnp.minimum(ahead, lax.rem(8 - ahead, 8))

    nearer = (gap(1) < gap(0)).astype(jnp.int32)

    exchange(PLUS)
    exchange(MINUS)
    round_0(0)
    act_send(PLUS, 0)
    act_send(MINUS, 0)
    hand_over(act_slot(z, c, 0), 0)
    hand_over(act_slot(z, c, 1), 1)
    acc[...] = jnp.zeros_like(acc)

    for fetch in fetches[6:]:
        fetch.wait()
    slots = lax.broadcasted_iota(jnp.int32, (SEQ, 128), 0)
    for kind, lens in enumerate((tlen, vlen)):
        value = jnp.dot(cots[kind], obasis[...], preferred_element_type=F32)
        for i in range(4):
            rows = value[i * SEQ : (i + 1) * SEQ]
            opart[2 * i + kind] = jnp.where(slots < lens[i], rows, 0.0)
    orecv[t] = opart[t]

    round_1(0)
    round_2(0)
    exchange_on(PLUS)
    exchange_on(MINUS)
    act_send(PLUS, 1)
    act_send(MINUS, 1)
    round_3(0)
    acts(0)
    round_4(0)
    exchanged(PLUS)
    exchanged(MINUS)
    round_0(1)
    acts(1)
    round_5(0)
    acts(2)
    round_1(1)
    acts(3)
    round_6(0)
    round_2(1)
    handed_own()
    handed(0, 1, 2, 3)
    near_tasks(0)
    round_3(1)
    acts(4)
    near_tasks(1)
    round_4(1)
    for sign in (PLUS, MINUS):
        w_arrive(1, 1, sign, 6)
    multiply(nearer, (1 - zh) * 4 + x)
    acts(5)
    handed(4, 5)
    near_tasks(2)
    round_5(1)
    acts(6)
    handed(6)
    for k in range(1, 8):
        to = lax.rem(t + k, 8)
        start(copy(opart.at[to], orecv.at[t], tsend, trecv, k - 1,
                   {"dp": dp, "tensor": to, "fsdp": y}))

    near_tasks(3)
    multiply(1 - nearer, (1 - zh) * 4 + x)
    for sign in (PLUS, MINUS):
        w_arrive(1, 0, sign, 6)
    round_6(1, (7, 8))
    side_tasks()

    round_6(1, (9,))
    multiply(0, (1 - zh) * 4 + lax.rem(x + 2, 4))

    for k in range(1, 8):
        slot = orecv.at[mod(t - k, 8)]
        copy(slot, slot, tsend, trecv, k - 1, at_z(z, peer)).wait_recv()
    total = orecv[0]
    for k in range(1, 8):
        total += orecv[k]
    osum[...] = total
    klass = zh * 4 + zl
    train_share = copy(osum, otr, tsend, trecv, 7, at_z(z, peer))
    val_shares = []
    for zz in range(2):
        val_shares.append(copy(osum, ova, tsend, trecv, 8 + zz,
                               {"dp": zz * 4 + x, "tensor": klass, "fsdp": y}))
    own_val = [(c == 1) & (zh == zz) & (t == klass) for zz in range(2)]

    @pl.when(c == 0)
    def _():
        train_share.start()
        otr[...] = osum[...]

    for zz in range(2):
        @pl.when((c == 1) & jnp.logical_not(own_val[zz]))
        def _():
            val_shares[zz].start()

        @pl.when(own_val[zz])
        def _():
            ova[...] = osum[...]

    def silu(v):
        return v / (1.0 + jnp.exp(-v))

    basis = ibasis[:, pl.ds(pl.multiple_of(zh * 640, 128), SPAN)]
    basis = jnp.concatenate([basis, basis], axis=0)
    hbuf[0 : SPAN - HALF] = jnp.zeros((SPAN - HALF, 256), BF16)
    hbuf[HALF:SPAN] = jnp.zeros((SPAN - HALF, 256), BF16)

    def project(half, n):
        tokens = pl.ds(pl.multiple_of(n * 256, 256), 256)
        hidden = silu(acc[half, 0:HALF, tokens]) * acc[half, HALF : 2 * HALF, tokens]
        hbuf[pl.ds(pl.multiple_of(zh * (SPAN - HALF), 16), HALF), :] = hidden.astype(BF16)
        value = jnp.dot(basis, hbuf[...], preferred_element_type=F32)
        proj[half, tokens, :] = value.T

    def last_task(n, carry):
        k = (1 - zh) * 4 + lax.rem(x + 2, 4)
        rows = jnp.concatenate([wf[k, i] for i in range(4)], axis=1)
        tokens = pl.ds(pl.multiple_of(n * 256, 256), 256)
        acc[1, :, tokens] += lax.dot_general(
            rows, xf[k, 1, n], (((1,), (1,)), ((), ())), preferred_element_type=F32)
        project(0, n)
        return carry

    lax.fori_loop(0, 2, last_task, 0)

    def last_half(n, carry):
        project(1, n)
        return carry

    lax.fori_loop(0, 2, last_half, 0)

    left = lax.broadcasted_iota(jnp.int32, (SEQ, 128), 1) < 64

    def message(zz, cc):
        train = proj[zz // 4, (zz % 4) * SEQ : (zz % 4 + 1) * SEQ, :]
        first = pl.multiple_of(256 + (2 * (zz % 2) + cc) * SEQ, SEQ)
        val = proj[(zz % 4) // 2, pl.ds(first, SEQ), :]
        return jnp.where(left, train, val)

    for zz in range(8):
        toward[zz] = message(zz, peer)
    start(copy(toward, given, tsend, trecv, 10, at_z(z, peer)))
    for zz in range(8):
        kept[zz] = message(zz, c)
    copy(given, given, tsend, trecv, 10, at_z(z, peer)).wait_recv()
    for zz in range(8):
        passed[zz] = (kept[zz] + given[zz]).astype(BF16)
    for k in (4, 3, 5, 2, 6, 1, 7):
        to = lax.rem(z + k, 8)
        start(copy(passed.at[to], irecv.at[z], tsend, trecv, 10 + k, at_z(to, c)))
    both = kept[z] + given[z]

    @pl.when(c == 1)
    def _():
        copy(otr, otr, tsend, trecv, 7, at_z(z, peer)).wait_recv()

    from_self = (zh == t // 4) & (t == lax.rem(t, 4) * 2 + 1)
    for zz in range(2):
        @pl.when((zh == zz) & jnp.logical_not(from_self))
        def _():
            copy(ova, ova, tsend, trecv, 8 + zz, at_z(z, peer)).wait_recv()

    for k in range(1, 8):
        slot = irecv.at[mod(z - k, 8)]
        copy(slot, slot, tsend, trecv, 10 + k, at_z(z, peer)).wait_recv()
    for k in range(1, 8):
        both += irecv[mod(z - k, 8)].astype(F32)

    def unit(o_ref, first):
        sketch = lax.dot_general(
            both, o_ref[...], (((0,), (0,)), ((), ())),
            precision=lax.Precision.HIGHEST, preferred_element_type=F32)[first : first + 64]
        return sketch * lax.rsqrt(jnp.sum(sketch * sketch, keepdims=True) + 1e-06)

    vbuf[x * 4 + y] = unit(ova, 64).astype(BF16)
    hops = [0, 1, 2, 1]
    plane = sorted(((a, b) for a in range(4) for b in range(4)),
                   key=lambda d: (hops[d[0]] + hops[d[1]], d))
    for dx, dy in plane[:0:-1]:
        start(copy(vbuf.at[x * 4 + y], vbuf.at[x * 4 + y], tsend, trecv, 17 + dx * 4 + dy,
                   at_xy(lax.rem(x + dx, 4), lax.rem(y + dy, 4))))
    tbuf[zl] = unit(otr, 0)
    for k in range(1, 4):
        start(copy(tbuf.at[zl], tbuf.at[zl], tsend, trecv, 32 + k,
                   at_z(zh * 4 + lax.rem(zl + k, 4), c)))
    for k in range(1, 4):
        slot = tbuf.at[mod(zl - k, 4)]
        copy(slot, slot, tsend, trecv, 32 + k, at_z(z, peer)).wait_recv()
    n = 18
    for dx in range(4):
        for dy in range(4):
            if dx or dy:
                slot = vbuf.at[mod(x - dx, 4) * 4 + mod(y - dy, 4)]
                copy(slot, slot, tsend, trecv, n, at_z(z, peer)).wait_recv()
                n += 1

    where_r = lax.broadcasted_iota(jnp.int32, (128, 128), 0)
    where_l = lax.broadcasted_iota(jnp.int32, (128, 128), 1)
    place = where_l == (where_r // 8) * 4 + (t // 4) * 64 + lax.rem(t, 4)
    blocks = [[] for _ in range(4)]
    for v in range(16):
        val = vbuf[v].astype(F32)
        for i in range(4):
            product = tbuf[i] * val
            parts = [product[8 * q : 8 * q + 8] for q in range(8)]
            while len(parts) > 1:
                parts = [parts[q] + parts[q + 1] for q in range(0, len(parts), 2)]
            blocks[i].append(parts[0])
    lines = []
    for i in range(4):
        dots = jnp.sum(jnp.concatenate(blocks[i], axis=0), axis=1, keepdims=True)
        dots = dots * jnp.sqrt(jnp.float32(64 * 128))
        lines.append(jnp.sum(jnp.where(place, dots, 0.0), axis=0, keepdims=True))
    row[...] = jnp.concatenate(lines + [jnp.zeros((4, 128), F32)], axis=0)
    for k in range(1, 8):
        to = lax.rem(t + k, 8)
        start(copy(row, obuf.at[t], tsend, trecv, 35 + k, {"dp": dp, "tensor": to, "fsdp": y}))
    obuf[t] = row[...]
    for k in range(1, 8):
        slot = obuf.at[mod(t - k, 8)]
        copy(slot, slot, tsend, trecv, 35 + k, at_z(z, peer)).wait_recv()
    scores = obuf[0]
    for k in range(1, 8):
        scores += obuf[k]
    out[...] = scores[0:4]

    for c_ in started:
        c_.wait_send()

    @pl.when(c == 0)
    def _():
        train_share.wait_send()

    for zz in range(2):
        @pl.when((c == 1) & jnp.logical_not(own_val[zz]))
        def _():
            val_shares[zz].wait_send()


def on_device(
    train_acts, val_acts, train_cot, val_cot, train_lengths, val_lengths,
    gate_weight, up_weight, in_basis, out_basis,
):
    vmem = pl.BlockSpec(memory_space=pltpu.VMEM)
    dma = pltpu.SemaphoreType.DMA
    return pl.pallas_call(
        body,
        out_shape=jax.ShapeDtypeStruct((4, 128), F32),
        in_specs=[pl.BlockSpec(memory_space=pl.ANY)] * 10,
        out_specs=vmem,
        scratch_shapes=[
            pltpu.SMEM((4,), jnp.int32),
            pltpu.SMEM((4,), jnp.int32),
            pltpu.VMEM((2, HALF, 128), BF16),
            pltpu.VMEM((2, 256, 512), BF16),
            pltpu.VMEM((64, 1376), BF16),
            pltpu.VMEM((512, 128), BF16),
            pltpu.VMEM((8, 4, 2 * HALF, 128), BF16),
            pltpu.VMEM((2, HALF, 128), BF16),
            pltpu.VMEM((8, 2, 2, 256, 512), BF16),
            pltpu.VMEM((2, 2 * HALF, 512), F32),
            pltpu.VMEM((SPAN, 256), BF16),
            pltpu.VMEM((2, 512, 128), F32),
            pltpu.VMEM((8, SEQ, 128), F32),
            pltpu.VMEM((8, SEQ, 128), F32),
            pltpu.VMEM((SEQ, 128), F32),
            pltpu.VMEM((SEQ, 128), F32),
            pltpu.VMEM((SEQ, 128), F32),
            pltpu.VMEM((8, SEQ, 128), F32),
            pltpu.VMEM((8, SEQ, 128), F32),
            pltpu.VMEM((8, SEQ, 128), F32),
            pltpu.VMEM((8, SEQ, 128), BF16),
            pltpu.VMEM((8, SEQ, 128), BF16),
            pltpu.VMEM((4, 64, 128), F32),
            pltpu.VMEM((16, 64, 128), BF16),
            pltpu.VMEM((8, 128), F32),
            pltpu.VMEM((8, 8, 128), F32),
            dma((80,)), dma((80,)),
            dma((18,)), dma((18,)),
            dma((16,)), dma((16,)),
            dma((43,)), dma((43,)),
            dma((12,)),
        ],
        compiler_params=pltpu.CompilerParams(
            collective_id=0, has_side_effects=True, vmem_limit_bytes=60 * 1024 * 1024
        ),
    )(train_lengths, val_lengths, gate_weight.T, up_weight.T, train_acts, val_acts,
      train_cot, val_cot, in_basis.T, out_basis)


def solution(mesh):
    rows = P(("dp", "fsdp"), "tensor")
    placed = (rows, rows, rows, rows, P(("dp", "fsdp")), P(("dp", "fsdp")), rows, rows,
              P("tensor", None), P("tensor", None))
    return jax.shard_map(
        on_device, mesh=mesh, in_specs=placed, out_specs=P(("dp", "fsdp"), None), check_vma=False
    )
```
